32 devices in a mesh: dp: 2 (over y), row: 4 (over z), col: 4 (over x, core).
Axes of the slice: x: 2, y: 2, z: 4, core: 2. Of those that a mesh axis runs over, the one named last changes fastest.
Arguments:
- hidden: bfloat16 [16384, 768], P(('dp', 'row', 'col')), may hold values from -6 to 6
- segments: int32 [16, 1024], P(('dp', 'row')), may hold values from 0 to 7, never falling along the last dimension, each value on 1 to 800 neighbouring positions
- query_weight: bfloat16 [768, 768], P('row', 'col'), may hold values from -0.21875 to 0.21875
- key_weight: bfloat16 [768, 768], P('row', 'col'), may hold values from -0.21875 to 0.21875
- value_weight: bfloat16 [768, 768], P('row', 'col'), may hold values from -0.21875 to 0.21875
- query_bias: float32 [768], P('col'), may hold values from -3 to 3
- value_bias: float32 [768], P('col'), may hold values from -3 to 3
- output_weight: bfloat16 [768, 768], P('row', 'col'), may hold values from -1.75 to 1.75
- output_bias: float32 [768], replicated, may hold values from -3 to 3
- first_gain: float32 [768], replicated, may hold values from 0.25 to 1.75
- first_shift: float32 [768], replicated, may hold values from -3 to 3
- inner_weight: bfloat16 [768, 3072], P('row', 'col'), may hold values from -0.21875 to 0.21875
- inner_bias: float32 [3072], P('col'), may hold values from -3 to 3
- outer_weight: bfloat16 [768, 3072], P('row', 'col'), may hold values from -0.15625 to 0.15625
- outer_bias: float32 [768], replicated, may hold values from -3 to 3
- second_gain: float32 [768], replicated, may hold values from 0.25 to 1.75
- second_shift: float32 [768], replicated, may hold values from -3 to 3
- upstream: bfloat16 [16384, 768], P(('dp', 'row', 'col')), may hold values from -6 to 6
Outputs:
- layer_out: bfloat16 [16384, 768], P(('dp', 'row', 'col'))
- grad_inputs: float32 [16384, 768], P(('dp', 'row', 'col'))
- grad_query: float32 [768, 768], P('row', 'col')
- grad_key: float32 [768, 768], P('row', 'col')
- grad_value: float32 [768, 768], P('row', 'col')
- grad_query_bias: float32 [768], P('col')
- grad_value_bias: float32 [768], P('col')
- grad_output: float32 [768, 768], P('row', 'col')
- grad_output_bias: float32 [768], replicated
- grad_gain_one: float32 [768], replicated
- grad_shift_one: float32 [768], replicated
- grad_inner: float32 [768, 3072], P('row', 'col')
- grad_inner_bias: float32 [3072], P('col')
- grad_outer: float32 [768, 3072], P('row', 'col')
- grad_outer_bias: float32 [768], replicated
- grad_gain_two: float32 [768], replicated
- grad_shift_two: float32 [768], replicated
The draws below stay inside these ranges and needn't reach their ends.
Inputs may be any that keep to these rules, and one draw needn't show every extreme that they name: `segments`: segment numbers never fall along a sequence; each document holds 1 to 800 tokens, and one of each sequence holds exactly 800.
All inputs are finite; a program needn't handle non-finite values.
Results may differ from the reference program's by a relative error of at most 0.02.
Values may be sent and summed in bfloat16 or wider, within the bound.
A program may use at most 128 MiB of HBM per device.

```python
import math
import jax
import jax.numpy as jnp
import numpy as np
from jax import lax

D = 768
HEADS = 12
HEAD_DIM = 64
FF = 3072
SEQ = 1024
DOC_MOST = 800
DOCS = 8
SEQS = 16
TOKENS = 16384


def block_levels(own_key, shape, split, smallest, high):
    def one(position, blocks):
        draws = jax.random.uniform(jax.random.fold_in(jax.random.fold_in(own_key, 6), position), (blocks,), jnp.float32, smallest / len(split), high / len(split))
        return jnp.repeat(jnp.exp(draws), shape[position] // blocks).reshape((-1,) + (1,) * (len(shape) - position - 1))

    loudness = one(*split[0])
    for cut in split[1:]:
        loudness = loudness * one(*cut)
    return loudness


def length_profile(number_of, total, limit, slope):
    weights = [(1 << 20) // math.isqrt(standing ** slope) + 1 for standing in range(2, number_of + 1)]
    surplus, counts = total - limit - (number_of - 1), [1] * (number_of - 1)
    while surplus > 0:
        candidates = [i for i in range(number_of - 1) if counts[i] < limit]
        whole, budget = sum([weights[i] for i in candidates]), surplus
        for i in candidates:
            extra = min(limit - counts[i], max(1, budget * weights[i] // whole), surplus)
            counts[i] = counts[i] + extra
            surplus = surplus - extra
    return np.array([limit] + counts)


def uneven_parts(own_key, number_of, total, most, slope):
    if number_of == 2:
        one = jax.random.randint(own_key, (), max(1, total - most), min(most, total - 1) + 1)
        return jnp.stack([one, total - one])
    tallies = jnp.asarray(length_profile(number_of, total, most, slope), jnp.int32)
    couples = (number_of - 1) // 2
    source_of, sink = tallies[1:1 + 2 * couples:2], tallies[2:2 + 2 * couples:2]
    margin = jnp.minimum(source_of - 1, most - sink)
    passed = jax.random.randint(jax.random.fold_in(own_key, 1), (couples,), 0, 1 << 20) % (margin + 1)
    tallies = tallies.at[1:1 + 2 * couples:2].set(source_of - passed).at[2:2 + 2 * couples:2].set(sink + passed)
    return tallies[jax.random.permutation(jax.random.fold_in(own_key, 2), number_of)]


def bell_draw(rng, shape, width, limit, shards=(), kind=jnp.bfloat16):
    loudness = block_levels(rng, shape, shards, -0.22, 0.18) if shards else 1.0
    values = jax.random.normal(rng, shape, jnp.float32) * width * loudness
    return jnp.minimum(jnp.maximum(values, -limit), limit).astype(kind)


def setup_inputs(seed: int = 0) -> dict:
    arg_keys = jax.random.split(jax.random.key(seed), 19)
    return {
        "hidden": bell_draw(arg_keys[0], (TOKENS, D), 1.0, 6.0, ((0, 32),)),
        "segments": jax.vmap(lambda own: jnp.searchsorted(jnp.cumsum(uneven_parts(own, DOCS, SEQ, DOC_MOST, 2)), jnp.arange(SEQ), side="right"))(jax.random.split(arg_keys[1], SEQS)).reshape((SEQS, SEQ)).astype(jnp.int32),
        "query_weight": bell_draw(arg_keys[2], (D, D), D ** -0.5, 0.21875, ((0, 4), (1, 4))),
        "key_weight": bell_draw(arg_keys[3], (D, D), D ** -0.5, 0.21875, ((0, 4), (1, 4))),
        "value_weight": bell_draw(arg_keys[4], (D, D), D ** -0.5, 0.21875, ((0, 4), (1, 4))),
        "query_bias": bell_draw(arg_keys[5], (D,), 0.5, 3.0, ((0, 4),), jnp.float32),
        "value_bias": bell_draw(arg_keys[6], (D,), 0.5, 3.0, ((0, 4),), jnp.float32),
        "output_weight": bell_draw(arg_keys[7], (D, D), (max(4, D // 64)) ** -0.5, 1.75, ((0, 4), (1, 4))),
        "output_bias": bell_draw(arg_keys[8], (D,), 0.5, 3.0, (), jnp.float32),
        "first_gain": jnp.clip(1.0 + 0.15 * jax.random.normal(arg_keys[9], (D,), jnp.float32), 0.25, 1.75),
        "first_shift": bell_draw(arg_keys[10], (D,), 0.5, 3.0, (), jnp.float32),
        "inner_weight": bell_draw(arg_keys[11], (D, FF), D ** -0.5, 0.21875, ((0, 4), (1, 4))),
        "inner_bias": bell_draw(arg_keys[12], (FF,), 0.5, 3.0, ((0, 4),), jnp.float32),
        "outer_weight": bell_draw(arg_keys[13], (D, FF), (FF // 2) ** -0.5, 0.15625, ((0, 4), (1, 4))),
        "outer_bias": bell_draw(arg_keys[14], (D,), 0.5, 3.0, (), jnp.float32),
        "second_gain": jnp.clip(1.0 + 0.15 * jax.random.normal(arg_keys[15], (D,), jnp.float32), 0.25, 1.75),
        "second_shift": bell_draw(arg_keys[16], (D,), 0.5, 3.0, (), jnp.float32),
        "upstream": bell_draw(arg_keys[17], (TOKENS, D), 1.0, 6.0, ((0, 32),)),
    }


@jax.custom_vjp
def low(v):
    return lax.optimization_barrier(v.astype(jnp.bfloat16)).astype(jnp.float32)

@jax.custom_vjp
def low_back(v):
    return v

def low_keep(v):
    return (low(v), None)

def low_pass(kept, grad):
    return (grad,)

def back_keep(v):
    return (v, None)

def back_low(kept, grad):
    return (low(grad),)
low.defvjp(low_keep, low_pass)
low_back.defvjp(back_keep, back_low)
EPS_NORM = 1e-12
NEG_FILL = -1e+30

def project(left, right):
    return jnp.dot(left, right, precision=lax.Precision.HIGHEST)

def layer_norm(values, gain, shift):
    means = lax.optimization_barrier(jnp.mean(values, axis=1, keepdims=True))
    centered = values - means
    variance = lax.optimization_barrier(jnp.mean(centered * centered, axis=1, keepdims=True))
    return centered * lax.rsqrt(variance + EPS_NORM) * gain + shift

def attend_sequence(item):
    query, keys, values, segment = item
    query_heads = query.reshape(SEQ, HEADS, HEAD_DIM)
    key_heads = keys.reshape(SEQ, HEADS, HEAD_DIM)
    value_heads = values.reshape(SEQ, HEADS, HEAD_DIM)
    scores = jnp.einsum('qhd,khd->hqk', query_heads, key_heads, precision=lax.Precision.HIGHEST) * HEAD_DIM ** (-0.5)
    scores = low_back(scores)
    same_doc = segment[:, None] == segment[None, :]
    scores = jnp.where(same_doc[None], scores, NEG_FILL)
    peak = lax.optimization_barrier(jnp.max(scores, axis=2, keepdims=True))
    expos = jnp.exp(scores - peak)
    probs = expos / lax.optimization_barrier(jnp.sum(expos, axis=2, keepdims=True))
    mixed = jnp.einsum('hqk,khd->qhd', low(probs), value_heads, precision=lax.Precision.HIGHEST)
    return mixed.reshape(SEQ, D)

def forward(hidden, query_weight, key_weight, value_weight, query_bias, value_bias, output_weight, output_bias, first_gain, first_shift, inner_weight, inner_bias, outer_weight, outer_bias, second_gain, second_shift, segments):
    query = low_back(low(project(hidden, query_weight) + query_bias))
    keys = low_back(low(project(hidden, key_weight)))
    values = low_back(low(project(hidden, value_weight) + value_bias))

    def by_sequence(block):
        return block.reshape(SEQS, SEQ, D)
    mixed = lax.map(jax.checkpoint(attend_sequence), (by_sequence(query), by_sequence(keys), by_sequence(values), segments))
    mixed = low_back(low(mixed.reshape(TOKENS, D)))
    branch = low_back(project(mixed, output_weight.T) + output_bias)
    first_out = layer_norm(hidden + branch, first_gain, first_shift)
    inner_pre = low_back(project(low(first_out), inner_weight) + inner_bias)
    activated = low(jax.nn.gelu(inner_pre, approximate=False))
    outer_branch = low_back(project(activated, outer_weight.T) + outer_bias)
    return layer_norm(first_out + outer_branch, second_gain, second_shift)

def reference(hidden, segments, query_weight, key_weight, value_weight, query_bias, value_bias, output_weight, output_bias, first_gain, first_shift, inner_weight, inner_bias, outer_weight, outer_bias, second_gain, second_shift, upstream):
    floats = [item.astype(jnp.float32) for item in (hidden, query_weight, key_weight, value_weight, query_bias, value_bias, output_weight, output_bias, first_gain, first_shift, inner_weight, inner_bias, outer_weight, outer_bias, second_gain, second_shift)]

    def apply_layer(*params):
        return forward(*params, segments)
    layer_out, pullback = jax.vjp(apply_layer, *floats)
    gradients = pullback(upstream.astype(jnp.float32))
    return (layer_out.astype(jnp.bfloat16), gradients[0], gradients[1], gradients[2], gradients[3], gradients[4], gradients[5], gradients[6], gradients[7], gradients[8], gradients[9], gradients[10], gradients[11], gradients[12], gradients[13], gradients[14], gradients[15])
```

```python
import functools

import jax
import jax.numpy as jnp
from jax import lax
from jax.experimental import pallas as pl
from jax.experimental.pallas import tpu as pltpu
from jax.sharding import PartitionSpec as P

HEAD_DIM = 64
EPS_NORM = 1e-12
NEG_FILL = -1e30
SCALE = HEAD_DIM ** (-0.5)
MESH = pl.DeviceIdType.MESH
BF16 = jnp.bfloat16
F32 = jnp.float32
TILE = 256
INV_SQRT2 = 0.7071067811865476
INV_SQRT_2PI = 0.3989422804014327


def dot(left, right, left_dim, right_dim):
    dims = (((left_dim,), (right_dim,)), ((), ()))
    return lax.dot_general(left, right, dims, preferred_element_type=F32)


def flip(index, mask):
    result, bit = index, 0
    while (1 << bit) <= mask:
        if (mask >> bit) & 1:
            result = result + (1 - 2 * lax.rem(index // (1 << bit), 2)) * (1 << bit)
        bit += 1
    return result


def rows_at(start, size):
    return pl.ds(pl.multiple_of(start, 16), size)


class Copies:
    def __init__(self, send_sem, recv_sem):
        self.send_sem, self.recv_sem, self.made = send_sem, recv_sem, []

    def new(self, src, dst, device):
        number = len(self.made)
        copy = pltpu.make_async_remote_copy(
            src_ref=src,
            dst_ref=dst,
            send_sem=self.send_sem.at[number],
            recv_sem=self.recv_sem.at[number],
            device_id=device,
            device_id_type=MESH,
        )
        self.made.append(copy)
        return copy

    def finish(self):
        for copy in self.made:
            copy.wait_send()


def layer_kernel(
    sizes,
    own_joint,
    own_inner,
    own_outer,
    hidden,
    upstream,
    seg_col,
    seg_row,
    own_bias,
    vectors,
    layer_out,
    grad_inputs,
    out_joint,
    out_inner,
    out_outer,
    out_shared,
    out_bias,
    w_joint,
    w_inner,
    w_outer,
    x_full,
    query,
    keys,
    values,
    log_sums,
    head_mixed,
    mixed,
    bias_full,
    first_normed,
    first_scale,
    first_rows,
    activated,
    gelu_slope,
    branch_two,
    branch_one,
    grad_heads,
    send_part,
    recv_part,
    q_turned,
    o_turned,
    dk_turned,
    dv_turned,
    g_joint,
    g_inner,
    g_outer,
    xy_recv,
    z_recv,
    f_send,
    f_recv,
    shared_sum,
    bias_sum,
    shared_pair,
    vec_x,
    vec_dp,
    vec_z,
    send_sem,
    recv_sem,
):
    dp_size, row_size = sizes
    grad_second = grad_inputs
    tokens, width = hidden.shape
    length = 2 * tokens
    block = own_joint.shape[0]
    half = block // 2
    heads = w_joint.shape[2] // (4 * HEAD_DIM)
    piece = heads * HEAD_DIM
    tiles, own_tiles = length // TILE, tokens // TILE
    width_tiles = width // TILE
    dp, row, col = (lax.axis_index(name) for name in ("dp", "row", "col"))
    core, mine = lax.rem(col, 2), col // 2
    other = 1 - mine
    side = lax.rem(dp, 2)
    partner = {"dp": dp, "row": row, "col": flip(col, 1)}
    x_peer = {"dp": dp, "row": row, "col": flip(col, 2)}
    y_peer = {"dp": flip(dp, 1), "row": row, "col": col}
    dp_peers = [{"dp": flip(dp, mask), "row": row, "col": col} for mask in range(1, dp_size)]
    z_peers = [{"dp": dp, "row": flip(row, mask), "col": col} for mask in range(1, row_size)]
    z_of = [flip(row, mask) for mask in range(row_size)]
    copies = Copies(send_sem, recv_sem)

    barrier = pltpu.get_barrier_semaphore()
    everyone = [partner, x_peer] + dp_peers + z_peers
    for peer in everyone:
        pl.semaphore_signal(barrier, inc=1, device_id=peer, device_id_type=MESH)
    pl.semaphore_wait(barrier, len(everyone))

    own_start, far_start = core * tokens, (1 - core) * tokens

    def half_rows(z, which):
        return rows_at(z * block + which * half, half)

    def block_rows(z):
        return rows_at(z * block, block)

    class Gather:
        def __init__(self, own, full):
            self.own, self.full = own, full
            source = own.at[rows_at(side * half, half)]
            spot = full.at[mine, half_rows(row, side)]
            self.z = [copies.new(source, spot, peer) for peer in z_peers]
            self.x_own = copies.new(own, full.at[mine, block_rows(row)], x_peer)
            got = [full.at[mine, half_rows(z, side)] for z in z_of[1:]]
            self.x = [copies.new(ref, ref, x_peer) for ref in got]
            self.y = [copies.new(ref, ref, y_peer) for ref in got]
            got = [full.at[other, half_rows(z, side)] for z in z_of[1:]]
            self.xy = [copies.new(ref, ref, y_peer) for ref in got]

        def start(self):
            self.z[0].start()
            self.x_own.start()

        def near(self):
            self.z[0].wait_recv()
            self.y[0].start()
            self.x[0].start()
            for copy in self.z[1:]:
                copy.start()

        def far(self):
            for z, x, y in list(zip(self.z, self.x, self.y))[1:]:
                z.wait_recv()
                y.start()
                x.start()

        def across(self):
            for x, xy in zip(self.x, self.xy):
                x.wait_recv()
                xy.start()

        def done(self):
            self.x_own.wait_recv()
            for copy in self.y + self.xy:
                copy.wait_recv()

    gathers = [
        Gather(own_joint, w_joint),
        Gather(own_inner, w_inner),
        Gather(own_outer, w_outer),
    ]
    gathers[0].start()
    own_rows_all = rows_at(own_start, tokens)
    send_x = copies.new(hidden, x_full.at[own_rows_all], partner)
    send_x.start()
    send_bias = copies.new(own_bias, bias_full.at[mine], x_peer)
    send_bias.start()
    for own, full in ((own_joint, w_joint), (own_inner, w_inner), (own_outer, w_outer)):
        full[mine, block_rows(row), :] = own[...]
    x_full[own_rows_all, :] = hidden[...]
    bias_full[mine] = own_bias[...]
    shared_sum[...] = jnp.zeros_like(shared_sum)
    bias_sum[...] = jnp.zeros_like(bias_sum)

    gathers[0].near()
    gathers[0].far()
    gathers[1].start()
    gathers[0].across()
    gathers[1].near()
    send_x.wait_recv()
    send_bias.wait_recv()
    gathers[0].done()

    def project(tile, carry):
        rows = rows_at(tile * TILE, TILE)
        x = x_full[rows, :]
        for h in range(2):
            out = dot(x, w_joint[h, :, 128:], 1, 0) + bias_full[h, 0:1, 128:]
            at = piece - 128
            for which, target in enumerate((query, keys, values)):
                for i in range(heads):
                    start = at + which * piece + i * HEAD_DIM
                    part = out[:, start : start + HEAD_DIM].astype(BF16)
                    if which == 0:
                        part = part * SCALE
                    target[h * heads + i, rows, :] = part.astype(BF16)
        return carry

    lax.fori_loop(0, tiles, project, 0)
    gathers[1].far()

    lanes = lax.broadcasted_iota(jnp.int32, (TILE, 128), 1)

    def attend(head):
        def body(tile, carry):
            rows = rows_at(tile * TILE, TILE)
            scores = dot(query[head, rows, :], keys[head], 1, 1)
            scores = jnp.where(seg_col[rows, :] == seg_row[...], scores, NEG_FILL)
            peak = jnp.max(scores, axis=1, keepdims=True)
            expos = jnp.exp(scores - peak)
            total = jnp.sum(expos, axis=1, keepdims=True)
            out = dot(expos.astype(BF16), values[head], 1, 0) / total
            head_mixed[head, rows, :] = out.astype(BF16)
            log_sums[rows, :] = jnp.where(lanes == head, peak + jnp.log(total), log_sums[rows, :])
            return carry

        lax.fori_loop(0, tiles, body, 0)

    services = [
        gathers[1].across,
        gathers[2].start,
        gathers[2].near,
        lambda: (gathers[1].done(), gathers[2].far()),
        gathers[2].across,
        lambda: None,
    ]
    for head in range(2 * heads):
        attend(head)
        services[min(head, len(services) - 1)]()

    def join(tile, carry):
        rows = rows_at(tile * TILE, TILE)
        for h in range(2):
            parts = [head_mixed[h * heads + i, rows, :] for i in range(heads)]
            mixed[h, rows, :] = jnp.concatenate(parts, axis=1)
        return carry

    lax.fori_loop(0, tiles, join, 0)

    class Exchange:
        def __init__(self, number, partial_of):
            self.partial_of = partial_of
            self.send = send_part.at[number % 2]
            self.recv = recv_part.at[number]
            self.copies = [
                copies.new(
                    self.send.at[pl.ds(i * TILE, TILE)],
                    self.recv.at[pl.ds(i * TILE, TILE)],
                    partner,
                )
                for i in range(own_tiles)
            ]

        def give(self):
            for i, copy in enumerate(self.copies):
                part = self.partial_of(rows_at(far_start + i * TILE, TILE))
                self.send[pl.ds(i * TILE, TILE), :] = part.astype(BF16)
                copy.start()

        def take(self, i):
            part = self.partial_of(rows_at(own_start + i * TILE, TILE))
            self.copies[i].wait_recv()
            return part + self.recv[pl.ds(i * TILE, TILE), :].astype(F32)

    class Share:
        def __init__(self, full):
            self.full = full
            spots = [full.at[rows_at(own_start + i * TILE, TILE)] for i in range(own_tiles)]
            self.copies = [copies.new(ref, ref, partner) for ref in spots]

        def put(self, i, tile_rows):
            self.full[rows_at(own_start + i * TILE, TILE), :] = tile_rows
            self.copies[i].start()

        def wait(self):
            for copy in self.copies:
                copy.wait_recv()

    def mean(v):
        return jnp.sum(v, axis=1, keepdims=True) * (1.0 / width)

    def normalize(v):
        centered = v - mean(v)
        inv_scale = lax.rsqrt(mean(centered * centered) + EPS_NORM)
        return centered * inv_scale, inv_scale

    def norm_backward(grads, normed, inv_scale, gain):
        scaled = grads * gain
        return inv_scale * (scaled - mean(scaled) - normed * mean(scaled * normed))

    def add_shared(index, v):
        shared_sum[index : index + 1, :] += jnp.sum(v, axis=0, keepdims=True)

    def mixed_partial(rows):
        return dot(mixed[0, rows, :], w_joint[0, :, :piece], 1, 1) + dot(
            mixed[1, rows, :], w_joint[1, :, :piece], 1, 1
        )

    leave_one = Exchange(0, mixed_partial)
    leave_one.give()
    share_first = Share(first_rows)
    for i in range(own_tiles):
        rows = pl.ds(i * TILE, TILE)
        branch = leave_one.take(i) + vectors[0:1, :]
        normed, inv_scale = normalize(hidden[rows, :].astype(F32) + branch)
        first_normed[rows, :] = normed
        first_scale[rows, :] = inv_scale
        out = normed * vectors[1:2, :] + vectors[2:3, :]
        share_first.put(i, out.astype(BF16))

    def inner(tile, start):
        rows = rows_at(start + tile * TILE, TILE)
        x = first_rows[rows, :]
        for h in range(2):
            pre = dot(x, w_inner[h], 1, 0) + bias_full[h, 1:2, :]
            below = 0.5 + 0.5 * lax.erf(pre * INV_SQRT2)
            density = INV_SQRT_2PI * jnp.exp(-0.5 * pre * pre)
            activated[h, rows, :] = (pre * below).astype(BF16)
            gelu_slope[h, rows, :] = (below + pre * density).astype(BF16)
        return start

    lax.fori_loop(0, own_tiles, inner, own_start)
    share_first.wait()
    lax.fori_loop(0, own_tiles, inner, far_start)
    gathers[2].done()

    def outer_partial(rows):
        return dot(activated[0, rows, :], w_outer[0], 1, 1) + dot(
            activated[1, rows, :], w_outer[1], 1, 1
        )

    leave_two = Exchange(1, outer_partial)
    leave_two.give()
    share_two = Share(branch_two)
    for i in range(own_tiles):
        rows = pl.ds(i * TILE, TILE)
        branch = leave_two.take(i) + vectors[3:4, :]
        normed, inv_scale = normalize(
            first_normed[rows, :] * vectors[1:2, :] + vectors[2:3, :] + branch
        )
        layer_out[rows, :] = (normed * vectors[4:5, :] + vectors[5:6, :]).astype(BF16)
        grads = upstream[rows, :].astype(F32)
        back = norm_backward(grads, normed, inv_scale, vectors[4:5, :])
        grad_second[rows, :] = back
        rounded = back.astype(BF16)
        share_two.put(i, rounded)
        add_shared(3, rounded.astype(F32))
        add_shared(4, grads * normed)
        add_shared(5, grads)
    share_two.wait()

    class Reduce:
        def __init__(self, number, grads, out, x_first):
            self.grads, self.out, self.x_first = grads, out, x_first
            self.pool = pool = xy_recv.at[number]
            self.late = late = [rows_at(width + z * half, half) for z in z_of]
            self.zr, self.fs, self.fr = z_recv.at[number], f_send.at[number], f_recv.at[number]
            away = 1 - side
            if x_first:
                self.first = [
                    copies.new(grads.at[other, block_rows(z)], pool.at[block_rows(z)], x_peer)
                    for z in z_of
                ]
                self.second = [
                    copies.new(
                        grads.at[mine, half_rows(z, away)],
                        pool.at[late[j]],
                        y_peer,
                    )
                    for j, z in enumerate(z_of)
                ]
            else:
                self.first = [
                    copies.new(
                        grads.at[h, half_rows(z, away)], pool.at[self.early(h, z)], y_peer
                    )
                    for h in (other, mine)
                    for z in z_of
                ]
                self.second = [
                    copies.new(
                        grads.at[other, half_rows(z, side)],
                        pool.at[late[j]],
                        x_peer,
                    )
                    for j, z in enumerate(z_of)
                ]
            self.third = [
                copies.new(
                    grads.at[mine, half_rows(z, side)],
                    self.zr.at[mask],
                    peer,
                )
                for mask, (z, peer) in enumerate(zip(z_of[1:], z_peers))
            ]
            self.fourth = [copies.new(self.fs, self.fr.at[dp], peer) for peer in dp_peers]
            self.order = list(range(1, row_size)) + [0]

        def early(self, h, z):
            return rows_at(h * (width // 2) + z * half, half)

        def start(self):
            for j in self.order:
                self.first[j].start()

        def start_rest(self):
            for j in self.order:
                self.first[row_size + j].start()

        def add(self, rows, h, recv):
            total = self.grads[h, rows, :].astype(F32) + recv.astype(F32)
            self.grads[h, rows, :] = total.astype(BF16)

        def go_second(self):
            for j in self.order:
                z = z_of[j]
                self.first[j].wait_recv()
                if self.x_first:
                    self.add(block_rows(z), mine, self.pool[block_rows(z), :])
                else:
                    self.add(half_rows(z, side), other, self.pool[self.early(other, z), :])
                self.second[j].start()

        def go_third(self):
            for j in self.order:
                z = z_of[j]
                rows = half_rows(z, side)
                if not self.x_first:
                    self.first[row_size + j].wait_recv()
                self.second[j].wait_recv()
                if self.x_first:
                    self.add(rows, mine, self.pool[self.late[j], :])
                else:
                    total = (
                        self.grads[mine, rows, :].astype(F32)
                        + self.pool[self.early(mine, z), :].astype(F32)
                        + self.pool[self.late[j], :].astype(F32)
                    )
                    self.grads[mine, rows, :] = total.astype(BF16)
                if j:
                    self.third[j - 1].start()

        def go_fourth(self):
            total = self.grads[mine, half_rows(row, side), :].astype(F32)
            for mask, copy in enumerate(self.third):
                copy.wait_recv()
                total = total + self.zr[mask].astype(F32)
            self.fs[...] = total.astype(BF16)
            for copy in self.fourth:
                copy.start()

        def done(self):
            for copy in self.fourth:
                copy.wait_recv()
            self.fr[dp] = self.fs[...]
            for which in range(2):
                total = self.fr[which].astype(F32)
                for index in range(which + 2, dp_size, 2):
                    total = total + self.fr[index].astype(F32)
                self.out[pl.ds(which * half, half), :] = total

    reduce_outer = Reduce(0, g_outer, out_outer, True)
    reduce_inner = Reduce(1, g_inner, out_inner, False)
    reduce_joint = Reduce(2, g_joint, out_joint, True)

    def weight_grad(target, rows_of, cols_of, h):
        def body(tile, carry):
            at = pl.ds(pl.multiple_of(tile * TILE, TILE), TILE)
            target[h, at, :] = dot(rows_of[:, at], cols_of[h], 0, 0).astype(BF16)
            return carry

        lax.fori_loop(0, width_tiles, body, 0)

    weight_grad(g_outer, branch_two, activated, other)
    reduce_outer.start()

    def back_inner(tile, carry):
        rows = rows_at(tile * TILE, TILE)
        g = branch_two[rows, :]
        for h in range(2):
            back = dot(g, w_outer[h], 1, 0) * gelu_slope[h, rows, :].astype(F32)
            rounded = back.astype(BF16)
            gelu_slope[h, rows, :] = rounded
            bias_sum[h, 1:2, :] += jnp.sum(rounded.astype(F32), axis=0, keepdims=True)
        return carry

    lax.fori_loop(0, tiles, back_inner, 0)

    def inner_back_partial(rows):
        return dot(gelu_slope[0, rows, :], w_inner[0], 1, 1) + dot(
            gelu_slope[1, rows, :], w_inner[1], 1, 1
        )

    back_one = Exchange(2, inner_back_partial)
    for copy in leave_one.copies:
        copy.wait_send()
    back_one.give()
    weight_grad(g_outer, branch_two, activated, mine)
    share_one = Share(branch_one)
    for i in range(own_tiles):
        rows = pl.ds(i * TILE, TILE)
        grads = back_one.take(i) + grad_second[rows, :]
        normed = first_normed[rows, :]
        back = norm_backward(grads, normed, first_scale[rows, :], vectors[1:2, :])
        grad_second[rows, :] = back
        rounded = back.astype(BF16)
        share_one.put(i, rounded)
        add_shared(0, rounded.astype(F32))
        add_shared(1, grads * normed)
        add_shared(2, grads)
    send_shared = copies.new(shared_sum, shared_pair, partner)
    send_shared.start()
    weight_grad(g_inner, first_rows, gelu_slope, other)
    reduce_inner.start()
    weight_grad(g_inner, first_rows, gelu_slope, mine)
    reduce_inner.start_rest()
    share_one.wait()

    def back_mixed(tile, carry):
        rows = rows_at(tile * TILE, TILE)
        g = branch_one[rows, :]
        for h in range(2):
            out = dot(g, w_joint[h, :, :piece], 1, 0)
            for i in range(heads):
                part = out[:, i * HEAD_DIM : (i + 1) * HEAD_DIM]
                grad_heads[h * heads + i, rows, :] = part.astype(BF16)
        return carry

    lax.fori_loop(0, tiles, back_mixed, 0)
    reduce_outer.go_second()

    def attend_back(head, carry):
        q_turned[...] = query[head].T
        o_turned[...] = grad_heads[head].T
        dk_turned[...] = jnp.zeros_like(dk_turned)
        dv_turned[...] = jnp.zeros_like(dv_turned)

        def body(tile, carry):
            rows = rows_at(tile * TILE, TILE)
            q, g = query[head, rows, :], grad_heads[head, rows, :]
            scores = dot(q, keys[head], 1, 1)
            scores = jnp.where(seg_col[rows, :] == seg_row[...], scores, NEG_FILL)
            log_sum = jnp.sum(
                jnp.where(lanes == head, log_sums[rows, :], 0.0), axis=1, keepdims=True
            )
            probs = jnp.exp(scores - log_sum)
            grad_probs = dot(g, values[head], 1, 1)
            inner_sum = jnp.sum(
                g.astype(F32) * head_mixed[head, rows, :].astype(F32), axis=1, keepdims=True
            )
            grad_scores = (probs * (grad_probs - inner_sum)).astype(BF16)
            dv_turned[...] += dot(o_turned[:, rows], probs.astype(BF16), 1, 0)
            dk_turned[...] += dot(q_turned[:, rows], grad_scores, 1, 0)
            query[head, rows, :] = (dot(grad_scores, keys[head], 1, 0) * SCALE).astype(BF16)
            return carry

        lax.fori_loop(0, tiles, body, 0)
        keys[head] = dk_turned[...].T.astype(BF16)
        values[head] = dv_turned[...].T.astype(BF16)
        return carry

    grad_rows = activated

    def gather_heads(h):
        def body(tile, carry):
            rows = rows_at(tile * TILE, TILE)
            parts = [jnp.zeros((TILE, piece), BF16)]
            for source in (query, keys, values):
                for i in range(heads):
                    parts.append(source[h * heads + i, rows, :])
            joined = jnp.concatenate(parts, axis=1)
            grad_rows[h, rows, :] = joined
            bias_sum[h, 0:1, :] += jnp.sum(joined.astype(F32), axis=0, keepdims=True)
            return carry

        lax.fori_loop(0, tiles, body, 0)

        def joint_grad(tile, carry):
            at = pl.ds(pl.multiple_of(tile * TILE, TILE), TILE)
            g_joint[h, at, :] = dot(x_full[:, at], grad_rows[h], 0, 0).astype(BF16)
            g_joint[h, at, :piece] = dot(branch_one[:, at], mixed[h], 0, 0).astype(BF16)
            return carry

        lax.fori_loop(0, width_tiles, joint_grad, 0)

    attend_back(other * heads, 0)
    reduce_outer.go_third()
    attend_back(other * heads + 1, 0)
    reduce_inner.go_second()
    lax.fori_loop(other * heads + 2, other * heads + heads, attend_back, 0)
    gather_heads(other)
    reduce_joint.start()
    reduce_outer.go_fourth()
    attend_back(mine * heads, 0)
    reduce_inner.go_third()
    attend_back(mine * heads + 1, 0)
    reduce_inner.go_fourth()
    reduce_outer.done()
    lax.fori_loop(mine * heads + 2, mine * heads + heads, attend_back, 0)
    gather_heads(mine)

    send_shared.wait_recv()
    vec_x_send, vec_x_recv = vec_x.at[0], vec_x.at[1]
    vec_x[0, :8, :] = shared_sum[...] + shared_pair[...]
    vec_x[0, 8:, :] = bias_sum[other]
    send_vec_x = copies.new(vec_x_send, vec_x_recv, x_peer)
    send_vec_x.start()

    reduce_joint.go_second()

    def input_partial(rows):
        return dot(grad_rows[0, rows, :], w_joint[0], 1, 1) + dot(
            grad_rows[1, rows, :], w_joint[1], 1, 1
        )

    back_two = Exchange(3, input_partial)
    for copy in leave_two.copies:
        copy.wait_send()
    back_two.give()

    send_vec_x.wait_recv()
    vec_dp[dp, :8, :] = vec_x[0, :8, :] + vec_x[1, :8, :]
    vec_dp[dp, 8:, :] = bias_sum[mine] + vec_x[1, 8:, :]
    send_vec_dp = [copies.new(vec_dp.at[dp], vec_dp.at[dp], peer) for peer in dp_peers]
    for copy in send_vec_dp:
        copy.start()

    reduce_inner.done()
    reduce_joint.go_third()
    for i in range(own_tiles):
        rows = pl.ds(i * TILE, TILE)
        grad_inputs[rows, :] = back_two.take(i) + grad_second[rows, :]

    for copy in send_vec_dp:
        copy.wait_recv()
    total = vec_dp[0]
    for index in range(1, dp_size):
        total = total + vec_dp[index]
    vec_z[row] = total
    send_vec_z = [copies.new(vec_z.at[row], vec_z.at[row], peer) for peer in z_peers]
    for copy in send_vec_z:
        copy.start()

    reduce_joint.go_fourth()
    for copy in send_vec_z:
        copy.wait_recv()
    total = vec_z[0]
    for index in range(1, row_size):
        total = total + vec_z[index]
    out_shared[...] = total[:8]
    out_bias[...] = total[8:]
    reduce_joint.done()

    waited = set(map(id, leave_one.copies + leave_two.copies))
    for copy in copies.made:
        if id(copy) not in waited:
            copy.wait_send()


def shards(
    mesh_shape,
    hidden,
    segments,
    query_weight,
    key_weight,
    value_weight,
    query_bias,
    value_bias,
    output_weight,
    output_bias,
    first_gain,
    first_shift,
    inner_weight,
    inner_bias,
    outer_weight,
    outer_bias,
    second_gain,
    second_shift,
    upstream,
):
    dp_size, row_size, col_size = mesh_shape
    tokens, width = hidden.shape
    length = segments.shape[1]
    block, piece = query_weight.shape
    hidden_units = inner_weight.shape[1]
    heads = piece // HEAD_DIM
    assert col_size == 4 and length == 2 * tokens and 4 * piece == width == hidden_units
    joint = jnp.concatenate([output_weight, query_weight, key_weight, value_weight], axis=1)
    none = jnp.zeros((piece,), F32)
    joint_bias = jnp.concatenate([none, query_bias, none, value_bias])
    own_bias = jnp.zeros((8, width), F32).at[0].set(joint_bias).at[1].set(inner_bias)
    vectors = jnp.stack(
        [output_bias, first_gain, first_shift, outer_bias, second_gain, second_shift]
        + [jnp.zeros_like(output_bias)] * 2
    )
    segment = lax.dynamic_index_in_dim(segments, lax.axis_index("col") // 2, 0, keepdims=True)
    seg_col = segment.reshape(length, 1)
    half = block // 2
    vmem = pl.BlockSpec(memory_space=pltpu.VMEM)

    def shape(dims, dtype):
        return jax.ShapeDtypeStruct(dims, dtype)

    per_head = pltpu.VMEM((2 * heads, length, HEAD_DIM), BF16)
    weights = pltpu.VMEM((2, width, width), BF16)
    scratch = [
        weights,
        weights,
        weights,
        pltpu.VMEM((length, width), BF16),
        per_head,
        per_head,
        per_head,
        pltpu.VMEM((length, 128), F32),
        per_head,
        pltpu.VMEM((2, length, piece), BF16),
        pltpu.VMEM((2, 8, width), F32),
        pltpu.VMEM((tokens, width), F32),
        pltpu.VMEM((tokens, 1), F32),
        pltpu.VMEM((length, width), BF16),
        pltpu.VMEM((2, length, width), BF16),
        pltpu.VMEM((2, length, width), BF16),
        pltpu.VMEM((length, width), BF16),
        pltpu.VMEM((length, width), BF16),
        per_head,
        pltpu.VMEM((2, tokens, width), BF16),
        pltpu.VMEM((4, tokens, width), BF16),
        pltpu.VMEM((HEAD_DIM, length), BF16),
        pltpu.VMEM((HEAD_DIM, length), BF16),
        pltpu.VMEM((HEAD_DIM, length), F32),
        pltpu.VMEM((HEAD_DIM, length), F32),
        weights,
        weights,
        weights,
        pltpu.VMEM((3, 3 * width // 2, width), BF16),
        pltpu.VMEM((3, row_size - 1, half, width), BF16),
        pltpu.VMEM((3, half, width), BF16),
        pltpu.VMEM((3, dp_size, half, width), BF16),
        pltpu.VMEM((8, width), F32),
        pltpu.VMEM((2, 8, width), F32),
        pltpu.VMEM((8, width), F32),
        pltpu.VMEM((2, 16, width), F32),
        pltpu.VMEM((dp_size, 16, width), F32),
        pltpu.VMEM((row_size, 16, width), F32),
        pltpu.SemaphoreType.DMA((256,)),
        pltpu.SemaphoreType.DMA((256,)),
    ]
    (
        layer_out,
        grad_inputs,
        grad_joint,
        grad_inner,
        grad_outer,
        shared,
        biases,
    ) = pl.pallas_call(
        functools.partial(layer_kernel, (dp_size, row_size)),
        out_shape=[
            shape((tokens, width), BF16),
            shape((tokens, width), F32),
            shape((block, width), F32),
            shape((block, width), F32),
            shape((block, width), F32),
            shape((8, width), F32),
            shape((8, width), F32),
        ],
        in_specs=[vmem] * 9,
        out_specs=[vmem] * 7,
        scratch_shapes=scratch,
        compiler_params=pltpu.CompilerParams(
            collective_id=0, has_side_effects=True, vmem_limit_bytes=67043328
        ),
        name="layer",
    )(
        joint,
        inner_weight,
        outer_weight,
        hidden,
        upstream,
        seg_col,
        segment,
        own_bias,
        vectors,
    )
    return (
        layer_out,
        grad_inputs,
        grad_joint[:, piece : 2 * piece],
        grad_joint[:, 2 * piece : 3 * piece],
        grad_joint[:, 3 * piece :],
        biases[0, piece : 2 * piece],
        biases[0, 3 * piece :],
        grad_joint[:, :piece],
        shared[0],
        shared[1],
        shared[2],
        grad_inner,
        biases[1],
        grad_outer,
        shared[3],
        shared[4],
        shared[5],
    )


def solution(mesh):
    tokens_spec = P(("dp", "row", "col"), None)
    weight_spec = P("row", "col")
    in_specs = (
        tokens_spec,
        P(("dp", "row"), None),
        weight_spec,
        weight_spec,
        weight_spec,
        P("col"),
        P("col"),
        weight_spec,
        P(),
        P(),
        P(),
        weight_spec,
        P("col"),
        weight_spec,
        P(),
        P(),
        P(),
        tokens_spec,
    )
    out_specs = (
        tokens_spec,
        tokens_spec,
        weight_spec,
        weight_spec,
        weight_spec,
        P("col"),
        P("col"),
        weight_spec,
        P(),
        P(),
        P(),
        weight_spec,
        P("col"),
        weight_spec,
        P(),
        P(),
        P(),
    )
    mesh_shape = (mesh.shape["dp"], mesh.shape["row"], mesh.shape["col"])
    return jax.shard_map(
        functools.partial(shards, mesh_shape),
        mesh=mesh,
        in_specs=in_specs,
        out_specs=out_specs,
        check_vma=False,
    )
```

```python
import functools

import jax
import jax.numpy as jnp
from jax import lax
from jax.experimental import pallas as pl
from jax.experimental.pallas import tpu as pltpu
from jax.sharding import PartitionSpec as P

HEAD_DIM = 64
EPS_NORM = 1e-12
NEG_FILL = -1e30
SCALE = HEAD_DIM ** (-0.5)
MESH = pl.DeviceIdType.MESH
BF16 = jnp.bfloat16
F32 = jnp.float32
TILE = 256
INV_SQRT2 = 0.7071067811865476
INV_SQRT_2PI = 0.3989422804014327


def dot(left, right, left_dim, right_dim):
    dims = (((left_dim,), (right_dim,)), ((), ()))
    return lax.dot_general(left, right, dims, preferred_element_type=F32)


def flip(index, mask):
    result, bit = index, 0
    while (1 << bit) <= mask:
        if (mask >> bit) & 1:
            result = result + (1 - 2 * lax.rem(index // (1 << bit), 2)) * (1 << bit)
        bit += 1
    return result


def row_of(ref):
    return ref[...].reshape(1, ref.shape[0])


def rows_at(start, size):
    return pl.ds(pl.multiple_of(start, 16), size)


class Copy:
    def __init__(self, descriptor):
        self.descriptor, self.started, self.sent = descriptor, False, False

    def start(self):
        self.descriptor.start()
        self.started = True

    def wait_recv(self):
        self.descriptor.wait_recv()

    def wait_send(self):
        if self.started and not self.sent:
            self.descriptor.wait_send()
            self.sent = True


class Copies:
    def __init__(self, send_sem, recv_sem):
        self.send_sem, self.recv_sem, self.made = send_sem, recv_sem, []

    def new(self, src, dst, device):
        number = len(self.made)
        copy = Copy(
            pltpu.make_async_remote_copy(
                src_ref=src,
                dst_ref=dst,
                send_sem=self.send_sem.at[number],
                recv_sem=self.recv_sem.at[number],
                device_id=device,
                device_id_type=MESH,
            )
        )
        self.made.append(copy)
        return copy

    def finish(self):
        for copy in self.made:
            copy.wait_send()


def layer_kernel(
    sizes,
    output_weight,
    query_weight,
    key_weight,
    value_weight,
    own_inner,
    own_outer,
    hidden,
    upstream,
    segments,
    query_bias,
    value_bias,
    inner_bias,
    output_bias,
    first_gain,
    first_shift,
    outer_bias,
    second_gain,
    second_shift,
    layer_out,
    grad_inputs,
    out_joint,
    out_inner,
    out_outer,
    out_shared,
    out_bias,
    own_joint,
    seg_col,
    seg_row,
    own_bias,
    w_joint,
    w_inner,
    w_outer,
    x_full,
    query,
    keys,
    values,
    log_sums,
    head_mixed,
    mixed,
    bias_full,
    first_normed,
    first_scale,
    first_rows,
    activated,
    gelu_slope,
    branch_two,
    branch_one,
    grad_heads,
    send_part,
    recv_part,
    q_turned,
    o_turned,
    dk_turned,
    dv_turned,
    g_joint,
    g_inner,
    g_outer,
    xy_recv,
    z_recv,
    f_send,
    f_recv,
    shared_sum,
    bias_sum,
    shared_pair,
    vec_x,
    vec_dp,
    vec_z,
    send_sem,
    recv_sem,
):
    dp_size, row_size = sizes
    grad_second = grad_inputs
    tokens, width = hidden.shape
    length = 2 * tokens
    block = own_joint.shape[0]
    half = block // 2
    heads = w_joint.shape[2] // (4 * HEAD_DIM)
    piece = heads * HEAD_DIM
    tiles, own_tiles = length // TILE, tokens // TILE
    width_tiles = width // TILE
    dp, row, col = (lax.axis_index(name) for name in ("dp", "row", "col"))
    core, mine = lax.rem(col, 2), col // 2
    other = 1 - mine
    side = lax.rem(dp, 2)
    partner = {"dp": dp, "row": row, "col": flip(col, 1)}
    x_peer = {"dp": dp, "row": row, "col": flip(col, 2)}
    y_peer = {"dp": flip(dp, 1), "row": row, "col": col}
    dp_peers = [{"dp": flip(dp, mask), "row": row, "col": col} for mask in range(1, dp_size)]
    z_peers = [{"dp": dp, "row": flip(row, mask), "col": col} for mask in range(1, row_size)]
    z_of = [flip(row, mask) for mask in range(row_size)]
    copies = Copies(send_sem, recv_sem)

    parts = [output_weight[...], query_weight[...], key_weight[...], value_weight[...]]
    own_joint[...] = jnp.concatenate(parts, axis=1)
    none = jnp.zeros((1, piece), F32)
    joint_bias = jnp.concatenate([none, row_of(query_bias), none, row_of(value_bias)], axis=1)
    rest = jnp.zeros((6, width), F32)
    own_bias[...] = jnp.concatenate([joint_bias, row_of(inner_bias), rest], axis=0)
    barrier = pltpu.get_barrier_semaphore()
    everyone = [partner, x_peer] + dp_peers + z_peers
    for peer in everyone:
        pl.semaphore_signal(barrier, inc=1, device_id=peer, device_id_type=MESH)
    pl.semaphore_wait(barrier, len(everyone))

    own_start, far_start = core * tokens, (1 - core) * tokens

    def half_rows(z, which):
        return rows_at(z * block + which * half, half)

    def block_rows(z):
        return rows_at(z * block, block)

    class Gather:
        def __init__(self, own, full):
            self.own, self.full = own, full
            source = own.at[rows_at(side * half, half)]
            spot = full.at[mine, half_rows(row, side)]
            self.z = [copies.new(source, spot, peer) for peer in z_peers]
            self.x_own = copies.new(own, full.at[mine, block_rows(row)], x_peer)
            got = [full.at[mine, half_rows(z, side)] for z in z_of[1:]]
            self.x = [copies.new(ref, ref, x_peer) for ref in got]
            self.y = [copies.new(ref, ref, y_peer) for ref in got]
            got = [full.at[other, half_rows(z, side)] for z in z_of[1:]]
            self.xy = [copies.new(ref, ref, y_peer) for ref in got]

        def start(self):
            self.z[0].start()
            self.x_own.start()

        def near(self):
            self.z[0].wait_recv()
            self.y[0].start()
            self.x[0].start()
            for copy in self.z[1:]:
                copy.start()

        def far(self):
            for z, x, y in list(zip(self.z, self.x, self.y))[1:]:
                z.wait_recv()
                y.start()
                x.start()

        def across(self):
            for x, xy in zip(self.x, self.xy):
                x.wait_recv()
                xy.start()

        def done(self):
            self.x_own.wait_recv()
            for copy in self.y + self.xy:
                copy.wait_recv()

    gathers = [
        Gather(own_joint, w_joint),
        Gather(own_inner, w_inner),
        Gather(own_outer, w_outer),
    ]
    gathers[0].start()
    own_rows_all = rows_at(own_start, tokens)
    send_x = copies.new(hidden, x_full.at[own_rows_all], partner)
    send_x.start()
    send_bias = copies.new(own_bias, bias_full.at[mine], x_peer)
    send_bias.start()
    for own, full in ((own_joint, w_joint), (own_inner, w_inner), (own_outer, w_outer)):
        full[mine, block_rows(row), :] = own[...]
    x_full[own_rows_all, :] = hidden[...]
    bias_full[mine] = own_bias[...]
    seg_row[...] = jnp.where(mine == 0, segments[0:1, :], segments[1:2, :]).astype(F32)
    seg_col[...] = jnp.broadcast_to(seg_row[...], (128, length)).T
    shared_sum[...] = jnp.zeros_like(shared_sum)
    bias_sum[...] = jnp.zeros_like(bias_sum)

    gathers[0].near()
    gathers[0].far()
    gathers[1].start()
    gathers[0].across()
    gathers[1].near()
    send_x.wait_recv()
    send_bias.wait_recv()
    gathers[0].done()

    def project(tile, carry):
        rows = rows_at(tile * TILE, TILE)
        x = x_full[rows, :]
        for h in range(2):
            out = dot(x, w_joint[h, :, 128:], 1, 0) + bias_full[h, 0:1, 128:]
            at = piece - 128
            for which, target in enumerate((query, keys, values)):
                for i in range(heads):
                    start = at + which * piece + i * HEAD_DIM
                    part = out[:, start : start + HEAD_DIM].astype(BF16)
                    if which == 0:
                        part = part * SCALE
                    target[h * heads + i, rows, :] = part.astype(BF16)
        return carry

    lax.fori_loop(0, tiles, project, 0)
    gathers[1].far()

    lanes = lax.broadcasted_iota(jnp.int32, (TILE, 128), 1)

    def attend(head):
        def body(tile, carry):
            rows = rows_at(tile * TILE, TILE)
            scores = dot(query[head, rows, :], keys[head], 1, 1)
            scores = jnp.where(seg_col[rows, 0:1] == seg_row[...], scores, NEG_FILL)
            peak = jnp.max(scores, axis=1, keepdims=True)
            expos = jnp.exp(scores - peak)
            total = jnp.sum(expos, axis=1, keepdims=True)
            out = dot(expos.astype(BF16), values[head], 1, 0) / total
            head_mixed[head, rows, :] = out.astype(BF16)
            log_sums[rows, :] = jnp.where(lanes == head, peak + jnp.log(total), log_sums[rows, :])
            return carry

        lax.fori_loop(0, tiles, body, 0)

    services = [
        gathers[1].across,
        gathers[2].start,
        gathers[2].near,
        lambda: (gathers[1].done(), gathers[2].far()),
        gathers[2].across,
        lambda: None,
    ]
    for head in range(2 * heads):
        attend(head)
        services[min(head, len(services) - 1)]()

    def join(tile, carry):
        rows = rows_at(tile * TILE, TILE)
        for h in range(2):
            parts = [head_mixed[h * heads + i, rows, :] for i in range(heads)]
            mixed[h, rows, :] = jnp.concatenate(parts, axis=1)
        return carry

    lax.fori_loop(0, tiles, join, 0)

    class Exchange:
        def __init__(self, number, partial_of):
            self.partial_of = partial_of
            self.send = send_part.at[number % 2]
            self.recv = recv_part.at[number]
            self.copies = [
                copies.new(
                    self.send.at[pl.ds(i * TILE, TILE)],
                    self.recv.at[pl.ds(i * TILE, TILE)],
                    partner,
                )
                for i in range(own_tiles)
            ]

        def give(self):
            for i, copy in enumerate(self.copies):
                part = self.partial_of(rows_at(far_start + i * TILE, TILE))
                self.send[pl.ds(i * TILE, TILE), :] = part.astype(BF16)
                copy.start()

        def take(self, i):
            part = self.partial_of(rows_at(own_start + i * TILE, TILE))
            self.copies[i].wait_recv()
            return part + self.recv[pl.ds(i * TILE, TILE), :].astype(F32)

    class Share:
        def __init__(self, full):
            self.full = full
            spots = [full.at[rows_at(own_start + i * TILE, TILE)] for i in range(own_tiles)]
            self.copies = [copies.new(ref, ref, partner) for ref in spots]

        def put(self, i, tile_rows):
            self.full[rows_at(own_start + i * TILE, TILE), :] = tile_rows
            self.copies[i].start()

        def wait(self):
            for copy in self.copies:
                copy.wait_recv()

    def mean(v):
        return jnp.sum(v, axis=1, keepdims=True) * (1.0 / width)

    def normalize(v):
        centered = v - mean(v)
        inv_scale = lax.rsqrt(mean(centered * centered) + EPS_NORM)
        return centered * inv_scale, inv_scale

    def norm_backward(grads, normed, inv_scale, gain):
        scaled = grads * gain
        return inv_scale * (scaled - mean(scaled) - normed * mean(scaled * normed))

    def add_shared(index, v):
        shared_sum[index : index + 1, :] += jnp.sum(v, axis=0, keepdims=True)

    def mixed_partial(rows):
        return dot(mixed[0, rows, :], w_joint[0, :, :piece], 1, 1) + dot(
            mixed[1, rows, :], w_joint[1, :, :piece], 1, 1
        )

    leave_one = Exchange(0, mixed_partial)
    leave_one.give()
    share_first = Share(first_rows)
    for i in range(own_tiles):
        rows = pl.ds(i * TILE, TILE)
        branch = leave_one.take(i) + row_of(output_bias)
        normed, inv_scale = normalize(hidden[rows, :].astype(F32) + branch)
        first_normed[rows, :] = normed
        first_scale[rows, :] = inv_scale
        out = normed * row_of(first_gain) + row_of(first_shift)
        share_first.put(i, out.astype(BF16))

    def inner(tile, start):
        rows = rows_at(start + tile * TILE, TILE)
        x = first_rows[rows, :]
        for h in range(2):
            pre = dot(x, w_inner[h], 1, 0) + bias_full[h, 1:2, :]
            below = 0.5 + 0.5 * lax.erf(pre * INV_SQRT2)
            density = INV_SQRT_2PI * jnp.exp(-0.5 * pre * pre)
            activated[h, rows, :] = (pre * below).astype(BF16)
            gelu_slope[h, rows, :] = (below + pre * density).astype(BF16)
        return start

    lax.fori_loop(0, own_tiles, inner, own_start)
    share_first.wait()
    lax.fori_loop(0, own_tiles, inner, far_start)
    gathers[2].done()

    def outer_partial(rows):
        return dot(activated[0, rows, :], w_outer[0], 1, 1) + dot(
            activated[1, rows, :], w_outer[1], 1, 1
        )

    leave_two = Exchange(1, outer_partial)
    leave_two.give()
    share_two = Share(branch_two)
    for i in range(own_tiles):
        rows = pl.ds(i * TILE, TILE)
        branch = leave_two.take(i) + row_of(outer_bias)
        normed, inv_scale = normalize(
            first_normed[rows, :] * row_of(first_gain) + row_of(first_shift) + branch
        )
        layer_out[rows, :] = (normed * row_of(second_gain) + row_of(second_shift)).astype(BF16)
        grads = upstream[rows, :].astype(F32)
        back = norm_backward(grads, normed, inv_scale, row_of(second_gain))
        grad_second[rows, :] = back
        rounded = back.astype(BF16)
        share_two.put(i, rounded)
        add_shared(3, rounded.astype(F32))
        add_shared(4, grads * normed)
        add_shared(5, grads)
    share_two.wait()

    class Reduce:
        def __init__(self, number, grads, out, x_first):
            self.grads, self.out, self.x_first = grads, out, x_first
            self.pool = pool = xy_recv.at[number]
            self.late = late = [rows_at(width + z * half, half) for z in z_of]
            self.zr, self.fs, self.fr = z_recv.at[number], f_send.at[number], f_recv.at[number]
            away = 1 - side
            if x_first:
                self.first = [
                    copies.new(grads.at[other, block_rows(z)], pool.at[block_rows(z)], x_peer)
                    for z in z_of
                ]
                self.second = [
                    copies.new(
                        grads.at[mine, half_rows(z, away)],
                        pool.at[late[j]],
                        y_peer,
                    )
                    for j, z in enumerate(z_of)
                ]
            else:
                self.first = [
                    copies.new(
                        grads.at[h, half_rows(z, away)], pool.at[self.early(h, z)], y_peer
                    )
                    for h in (other, mine)
                    for z in z_of
                ]
                self.second = [
                    copies.new(
                        grads.at[other, half_rows(z, side)],
                        pool.at[late[j]],
                        x_peer,
                    )
                    for j, z in enumerate(z_of)
                ]
            self.third = [
                copies.new(
                    grads.at[mine, half_rows(z, side)],
                    self.zr.at[mask],
                    peer,
                )
                for mask, (z, peer) in enumerate(zip(z_of[1:], z_peers))
            ]
            self.fourth = [copies.new(self.fs, self.fr.at[dp], peer) for peer in dp_peers]
            self.order = list(range(1, row_size)) + [0]

        def early(self, h, z):
            return rows_at(h * (width // 2) + z * half, half)

        def start(self):
            for j in self.order:
                self.first[j].start()

        def start_rest(self):
            for j in self.order:
                self.first[row_size + j].start()

        def add(self, rows, h, recv):
            total = self.grads[h, rows, :].astype(F32) + recv.astype(F32)
            self.grads[h, rows, :] = total.astype(BF16)

        def go_second(self):
            for j in self.order:
                z = z_of[j]
                self.first[j].wait_recv()
                if self.x_first:
                    self.add(block_rows(z), mine, self.pool[block_rows(z), :])
                else:
                    self.add(half_rows(z, side), other, self.pool[self.early(other, z), :])
                self.second[j].start()

        def go_third(self):
            for j in self.order:
                z = z_of[j]
                rows = half_rows(z, side)
                if not self.x_first:
                    self.first[row_size + j].wait_recv()
                self.second[j].wait_recv()
                if self.x_first:
                    self.add(rows, mine, self.pool[self.late[j], :])
                else:
                    total = (
                        self.grads[mine, rows, :].astype(F32)
                        + self.pool[self.early(mine, z), :].astype(F32)
                        + self.pool[self.late[j], :].astype(F32)
                    )
                    self.grads[mine, rows, :] = total.astype(BF16)
                if j:
                    self.third[j - 1].start()

        def go_fourth(self):
            total = self.grads[mine, half_rows(row, side), :].astype(F32)
            for mask, copy in enumerate(self.third):
                copy.wait_recv()
                total = total + self.zr[mask].astype(F32)
            self.fs[...] = total.astype(BF16)
            for copy in self.fourth:
                copy.start()

        def done(self):
            for copy in self.fourth:
                copy.wait_recv()
            self.fr[dp] = self.fs[...]
            for which in range(2):
                total = self.fr[which].astype(F32)
                for index in range(which + 2, dp_size, 2):
                    total = total + self.fr[index].astype(F32)
                self.out[pl.ds(which * half, half), :] = total

    reduce_outer = Reduce(0, g_outer, out_outer, True)
    reduce_inner = Reduce(1, g_inner, out_inner, False)
    reduce_joint = Reduce(2, g_joint, out_joint, True)

    def weight_grad(target, rows_of, cols_of, h):
        def body(tile, carry):
            at = pl.ds(pl.multiple_of(tile * TILE, TILE), TILE)
            target[h, at, :] = dot(rows_of[:, at], cols_of[h], 0, 0).astype(BF16)
            return carry

        lax.fori_loop(0, width_tiles, body, 0)

    weight_grad(g_outer, branch_two, activated, other)
    reduce_outer.start()

    def back_inner(tile, carry):
        rows = rows_at(tile * TILE, TILE)
        g = branch_two[rows, :]
        for h in range(2):
            back = dot(g, w_outer[h], 1, 0) * gelu_slope[h, rows, :].astype(F32)
            rounded = back.astype(BF16)
            gelu_slope[h, rows, :] = rounded
            bias_sum[h, 1:2, :] += jnp.sum(rounded.astype(F32), axis=0, keepdims=True)
        return carry

    lax.fori_loop(0, tiles, back_inner, 0)

    def inner_back_partial(rows):
        return dot(gelu_slope[0, rows, :], w_inner[0], 1, 1) + dot(
            gelu_slope[1, rows, :], w_inner[1], 1, 1
        )

    back_one = Exchange(2, inner_back_partial)
    for copy in leave_one.copies:
        copy.wait_send()
    back_one.give()
    weight_grad(g_outer, branch_two, activated, mine)
    share_one = Share(branch_one)
    for i in range(own_tiles):
        rows = pl.ds(i * TILE, TILE)
        grads = back_one.take(i) + grad_second[rows, :]
        normed = first_normed[rows, :]
        back = norm_backward(grads, normed, first_scale[rows, :], row_of(first_gain))
        grad_second[rows, :] = back
        rounded = back.astype(BF16)
        share_one.put(i, rounded)
        add_shared(0, rounded.astype(F32))
        add_shared(1, grads * normed)
        add_shared(2, grads)
    send_shared = copies.new(shared_sum, shared_pair, partner)
    send_shared.start()
    weight_grad(g_inner, first_rows, gelu_slope, other)
    reduce_inner.start()
    weight_grad(g_inner, first_rows, gelu_slope, mine)
    reduce_inner.start_rest()
    share_one.wait()

    def back_mixed(tile, carry):
        rows = rows_at(tile * TILE, TILE)
        g = branch_one[rows, :]
        for h in range(2):
            out = dot(g, w_joint[h, :, :piece], 1, 0)
            for i in range(heads):
                part = out[:, i * HEAD_DIM : (i + 1) * HEAD_DIM]
                grad_heads[h * heads + i, rows, :] = part.astype(BF16)
        return carry

    lax.fori_loop(0, tiles, back_mixed, 0)
    reduce_outer.go_second()

    def attend_back(head, carry):
        q_turned[...] = query[head].T
        o_turned[...] = grad_heads[head].T
        dk_turned[...] = jnp.zeros_like(dk_turned)
        dv_turned[...] = jnp.zeros_like(dv_turned)

        def body(tile, carry):
            rows = rows_at(tile * TILE, TILE)
            q, g = query[head, rows, :], grad_heads[head, rows, :]
            scores = dot(q, keys[head], 1, 1)
            scores = jnp.where(seg_col[rows, 0:1] == seg_row[...], scores, NEG_FILL)
            log_sum = jnp.sum(
                jnp.where(lanes == head, log_sums[rows, :], 0.0), axis=1, keepdims=True
            )
            probs = jnp.exp(scores - log_sum)
            grad_probs = dot(g, values[head], 1, 1)
            inner_sum = jnp.sum(
                g.astype(F32) * head_mixed[head, rows, :].astype(F32), axis=1, keepdims=True
            )
            grad_scores = (probs * (grad_probs - inner_sum)).astype(BF16)
            dv_turned[...] += dot(o_turned[:, rows], probs.astype(BF16), 1, 0)
            dk_turned[...] += dot(q_turned[:, rows], grad_scores, 1, 0)
            query[head, rows, :] = (dot(grad_scores, keys[head], 1, 0) * SCALE).astype(BF16)
            return carry

        lax.fori_loop(0, tiles, body, 0)
        keys[head] = dk_turned[...].T.astype(BF16)
        values[head] = dv_turned[...].T.astype(BF16)
        return carry

    grad_rows = activated

    def gather_heads(h):
        def body(tile, carry):
            rows = rows_at(tile * TILE, TILE)
            parts = [jnp.zeros((TILE, piece), BF16)]
            for source in (query, keys, values):
                for i in range(heads):
                    parts.append(source[h * heads + i, rows, :])
            joined = jnp.concatenate(parts, axis=1)
            grad_rows[h, rows, :] = joined
            bias_sum[h, 0:1, :] += jnp.sum(joined.astype(F32), axis=0, keepdims=True)
            return carry

        lax.fori_loop(0, tiles, body, 0)

        def joint_grad(tile, carry):
            at = pl.ds(pl.multiple_of(tile * TILE, TILE), TILE)
            g_joint[h, at, :] = dot(x_full[:, at], grad_rows[h], 0, 0).astype(BF16)
            g_joint[h, at, :piece] = dot(branch_one[:, at], mixed[h], 0, 0).astype(BF16)
            return carry

        lax.fori_loop(0, width_tiles, joint_grad, 0)

    attend_back(other * heads, 0)
    reduce_outer.go_third()
    attend_back(other * heads + 1, 0)
    reduce_inner.go_second()
    lax.fori_loop(other * heads + 2, other * heads + heads, attend_back, 0)
    gather_heads(other)
    reduce_joint.start()
    reduce_outer.go_fourth()
    attend_back(mine * heads, 0)
    reduce_inner.go_third()
    attend_back(mine * heads + 1, 0)
    reduce_inner.go_fourth()
    reduce_outer.done()
    lax.fori_loop(mine * heads + 2, mine * heads + heads, attend_back, 0)
    gather_heads(mine)

    send_shared.wait_recv()
    vec_x_send, vec_x_recv = vec_x.at[0], vec_x.at[1]
    vec_x[0, :8, :] = shared_sum[...] + shared_pair[...]
    vec_x[0, 8:, :] = bias_sum[other]
    send_vec_x = copies.new(vec_x_send, vec_x_recv, x_peer)
    send_vec_x.start()

    reduce_joint.go_second()

    def input_partial(rows):
        return dot(grad_rows[0, rows, :], w_joint[0], 1, 1) + dot(
            grad_rows[1, rows, :], w_joint[1], 1, 1
        )

    back_two = Exchange(3, input_partial)
    for copy in leave_two.copies:
        copy.wait_send()
    back_two.give()

    send_vec_x.wait_recv()
    vec_dp[dp, :8, :] = vec_x[0, :8, :] + vec_x[1, :8, :]
    vec_dp[dp, 8:, :] = bias_sum[mine] + vec_x[1, 8:, :]
    send_vec_dp = [copies.new(vec_dp.at[dp], vec_dp.at[dp], peer) for peer in dp_peers]
    for copy in send_vec_dp:
        copy.start()

    reduce_inner.done()
    reduce_joint.go_third()
    for i in range(own_tiles):
        rows = pl.ds(i * TILE, TILE)
        grad_inputs[rows, :] = back_two.take(i) + grad_second[rows, :]

    for copy in send_vec_dp:
        copy.wait_recv()
    total = vec_dp[0]
    for index in range(1, dp_size):
        total = total + vec_dp[index]
    vec_z[row] = total
    send_vec_z = [copies.new(vec_z.at[row], vec_z.at[row], peer) for peer in z_peers]
    for copy in send_vec_z:
        copy.start()

    reduce_joint.go_fourth()
    for copy in send_vec_z:
        copy.wait_recv()
    total = vec_z[0]
    for index in range(1, row_size):
        total = total + vec_z[index]
    out_shared[...] = total[:8]
    out_bias[...] = total[8:]
    reduce_joint.done()

    copies.finish()


def unpack_kernel(
    layer_in,
    inputs_in,
    joint_in,
    inner_in,
    outer_in,
    shared_in,
    bias_in,
    layer_out,
    inputs_out,
    query_out,
    key_out,
    value_out,
    output_out,
    inner_out,
    outer_out,
    query_bias_out,
    value_bias_out,
    *vectors_out,
):
    piece, width = query_out.shape[1], joint_in.shape[1]
    layer_out[...] = layer_in[...]
    inputs_out[...] = inputs_in[...]
    inner_out[...] = inner_in[...]
    outer_out[...] = outer_in[...]
    joint = joint_in[...]
    for which, out in enumerate((output_out, query_out, key_out, value_out)):
        out[...] = joint[:, which * piece : (which + 1) * piece]

    @pl.when(pl.program_id(0) == 0)
    def _():
        bias = bias_in[0:1, :]
        query_bias_out[...] = bias[:, piece : 2 * piece].reshape(piece)
        value_bias_out[...] = bias[:, 3 * piece :].reshape(piece)
        for index in range(6):
            vectors_out[index][...] = shared_in[index : index + 1, :].reshape(width)
        vectors_out[6][...] = bias_in[1:2, :].reshape(width)


def shards(
    mesh_shape,
    hidden,
    segments,
    query_weight,
    key_weight,
    value_weight,
    query_bias,
    value_bias,
    output_weight,
    output_bias,
    first_gain,
    first_shift,
    inner_weight,
    inner_bias,
    outer_weight,
    outer_bias,
    second_gain,
    second_shift,
    upstream,
):
    dp_size, row_size, col_size = mesh_shape
    tokens, width = hidden.shape
    length = segments.shape[1]
    block, piece = query_weight.shape
    hidden_units = inner_weight.shape[1]
    heads = piece // HEAD_DIM
    assert col_size == 4 and length == 2 * tokens and 4 * piece == width == hidden_units
    half = block // 2
    vmem = pl.BlockSpec(memory_space=pltpu.VMEM)

    def shape(dims, dtype):
        return jax.ShapeDtypeStruct(dims, dtype)

    per_head = pltpu.VMEM((2 * heads, length, HEAD_DIM), BF16)
    weights = pltpu.VMEM((2, width, width), BF16)
    scratch = [
        pltpu.VMEM((block, width), BF16),
        pltpu.VMEM((length, 128), F32),
        pltpu.VMEM((1, length), F32),
        pltpu.VMEM((8, width), F32),
        weights,
        weights,
        weights,
        pltpu.VMEM((length, width), BF16),
        per_head,
        per_head,
        per_head,
        pltpu.VMEM((length, 128), F32),
        per_head,
        pltpu.VMEM((2, length, piece), BF16),
        pltpu.VMEM((2, 8, width), F32),
        pltpu.VMEM((tokens, width), F32),
        pltpu.VMEM((tokens, 1), F32),
        pltpu.VMEM((length, width), BF16),
        pltpu.VMEM((2, length, width), BF16),
        pltpu.VMEM((2, length, width), BF16),
        pltpu.VMEM((length, width), BF16),
        pltpu.VMEM((length, width), BF16),
        per_head,
        pltpu.VMEM((2, tokens, width), BF16),
        pltpu.VMEM((4, tokens, width), BF16),
        pltpu.VMEM((HEAD_DIM, length), BF16),
        pltpu.VMEM((HEAD_DIM, length), BF16),
        pltpu.VMEM((HEAD_DIM, length), F32),
        pltpu.VMEM((HEAD_DIM, length), F32),
        weights,
        weights,
        weights,
        pltpu.VMEM((3, 3 * width // 2, width), BF16),
        pltpu.VMEM((3, row_size - 1, half, width), BF16),
        pltpu.VMEM((3, half, width), BF16),
        pltpu.VMEM((3, dp_size, half, width), BF16),
        pltpu.VMEM((8, width), F32),
        pltpu.VMEM((2, 8, width), F32),
        pltpu.VMEM((8, width), F32),
        pltpu.VMEM((2, 16, width), F32),
        pltpu.VMEM((dp_size, 16, width), F32),
        pltpu.VMEM((row_size, 16, width), F32),
        pltpu.SemaphoreType.DMA((256,)),
        pltpu.SemaphoreType.DMA((256,)),
    ]
    results = pl.pallas_call(
        functools.partial(layer_kernel, (dp_size, row_size)),
        out_shape=[
            shape((tokens, width), BF16),
            shape((tokens, width), F32),
            shape((block, width), F32),
            shape((block, width), F32),
            shape((block, width), F32),
            shape((8, width), F32),
            shape((8, width), F32),
        ],
        in_specs=[vmem] * 18,
        out_specs=[vmem] * 7,
        scratch_shapes=scratch,
        compiler_params=pltpu.CompilerParams(
            collective_id=0, has_side_effects=True, vmem_limit_bytes=67043328
        ),
        name="layer",
    )(
        output_weight,
        query_weight,
        key_weight,
        value_weight,
        inner_weight,
        outer_weight,
        hidden,
        upstream,
        segments,
        query_bias,
        value_bias,
        inner_bias,
        output_bias,
        first_gain,
        first_shift,
        outer_bias,
        second_gain,
        second_shift,
    )
    steps = 4

    def part(rows, columns):
        return pl.BlockSpec((rows // steps, columns), lambda i: (i, 0))

    def all_of(rows, columns):
        return pl.BlockSpec((rows, columns), lambda i: (0, 0))

    big = [part(tokens, width)] * 2
    small = [part(block, piece)] * 4
    square = [part(block, width)] * 2
    outs = pl.pallas_call(
        unpack_kernel,
        grid=(steps,),
        out_shape=[shape((tokens, width), BF16), shape((tokens, width), F32)]
        + [shape((block, piece), F32)] * 4
        + [shape((block, width), F32)] * 2
        + [shape((piece,), F32)] * 2
        + [shape((width,), F32)] * 7,
        in_specs=big + [part(block, width)] + square + [all_of(8, width)] * 2,
        out_specs=big + small + square + [pl.BlockSpec((piece,), lambda i: (0,))] * 2
        + [pl.BlockSpec((width,), lambda i: (0,))] * 7,
        name="unpack",
    )(*results)
    layer_out, grad_inputs, grad_query, grad_key, grad_value, grad_output = outs[:6]
    grad_inner, grad_outer = outs[6:8]
    vectors = outs[8:]
    return (
        layer_out,
        grad_inputs,
        grad_query,
        grad_key,
        grad_value,
        vectors[0],
        vectors[1],
        grad_output,
        vectors[2],
        vectors[3],
        vectors[4],
        grad_inner,
        vectors[8],
        grad_outer,
        vectors[5],
        vectors[6],
        vectors[7],
    )


def solution(mesh):
    tokens_spec = P(("dp", "row", "col"), None)
    weight_spec = P("row", "col")
    in_specs = (
        tokens_spec,
        P(("dp", "row"), None),
        weight_spec,
        weight_spec,
        weight_spec,
        P("col"),
        P("col"),
        weight_spec,
        P(),
        P(),
        P(),
        weight_spec,
        P("col"),
        weight_spec,
        P(),
        P(),
        P(),
        tokens_spec,
    )
    out_specs = (
        tokens_spec,
        tokens_spec,
        weight_spec,
        weight_spec,
        weight_spec,
        P("col"),
        P("col"),
        weight_spec,
        P(),
        P(),
        P(),
        weight_spec,
        P("col"),
        weight_spec,
        P(),
        P(),
        P(),
    )
    mesh_shape = (mesh.shape["dp"], mesh.shape["row"], mesh.shape["col"])
    return jax.shard_map(
        functools.partial(shards, mesh_shape),
        mesh=mesh,
        in_specs=in_specs,
        out_specs=out_specs,
        check_vma=False,
    )
```

```python
import functools

import jax
import jax.numpy as jnp
from jax import lax
from jax.experimental import pallas as pl
from jax.experimental.pallas import tpu as pltpu
from jax.sharding import PartitionSpec as P

HEAD_DIM = 64
EPS_NORM = 1e-12
NEG_FILL = -1e30
SCALE = HEAD_DIM ** (-0.5)
MESH = pl.DeviceIdType.MESH
BF16 = jnp.bfloat16
F32 = jnp.float32
TILE = 256
INV_SQRT2 = 0.7071067811865476
INV_SQRT_2PI = 0.3989422804014327


def dot(left, right, left_dim, right_dim):
    dims = (((left_dim,), (right_dim,)), ((), ()))
    return lax.dot_general(left, right, dims, preferred_element_type=F32)


def flip(index, mask):
    result, bit = index, 0
    while (1 << bit) <= mask:
        if (mask >> bit) & 1:
            result = result + (1 - 2 * lax.rem(index // (1 << bit), 2)) * (1 << bit)
        bit += 1
    return result


def row_of(ref):
    return ref[...].reshape(1, ref.shape[0])


def rows_at(start, size):
    return pl.ds(pl.multiple_of(start, 16), size)


class Copy:
    def __init__(self, descriptor):
        self.descriptor, self.started, self.sent = descriptor, False, False

    def start(self):
        self.descriptor.start()
        self.started = True

    def wait_recv(self):
        self.descriptor.wait_recv()

    def wait_send(self):
        if self.started and not self.sent:
            self.descriptor.wait_send()
            self.sent = True


class Copies:
    def __init__(self, send_sem, recv_sem):
        self.send_sem, self.recv_sem, self.made = send_sem, recv_sem, []

    def new(self, src, dst, device):
        number = len(self.made)
        copy = Copy(
            pltpu.make_async_remote_copy(
                src_ref=src,
                dst_ref=dst,
                send_sem=self.send_sem.at[number],
                recv_sem=self.recv_sem.at[number],
                device_id=device,
                device_id_type=MESH,
            )
        )
        self.made.append(copy)
        return copy

    def finish(self):
        for copy in self.made:
            copy.wait_send()


def layer_kernel(
    sizes,
    output_weight,
    query_weight,
    key_weight,
    value_weight,
    own_inner,
    own_outer,
    hidden,
    upstream,
    segments,
    query_bias,
    value_bias,
    inner_bias,
    output_bias,
    first_gain,
    first_shift,
    outer_bias,
    second_gain,
    second_shift,
    layer_hbm,
    inputs_hbm,
    joint_hbm,
    inner_hbm,
    outer_hbm,
    out_shared,
    out_bias,
    layer_out,
    grad_inputs,
    out_joint,
    out_inner,
    out_outer,
    store_sem,
    own_joint,
    seg_col,
    seg_row,
    own_bias,
    w_joint,
    w_inner,
    w_outer,
    x_full,
    query,
    keys,
    values,
    log_sums,
    head_mixed,
    mixed,
    bias_full,
    first_normed,
    first_scale,
    first_rows,
    activated,
    gelu_slope,
    branch_two,
    branch_one,
    grad_heads,
    send_part,
    recv_part,
    q_turned,
    o_turned,
    dk_turned,
    dv_turned,
    g_joint,
    g_inner,
    g_outer,
    xy_recv,
    z_recv,
    f_send,
    f_recv,
    shared_sum,
    bias_sum,
    shared_pair,
    vec_x,
    vec_dp,
    vec_z,
    send_sem,
    recv_sem,
):
    dp_size, row_size = sizes
    grad_second = grad_inputs
    tokens, width = hidden.shape
    length = 2 * tokens
    block = own_joint.shape[0]
    half = block // 2
    heads = w_joint.shape[2] // (4 * HEAD_DIM)
    piece = heads * HEAD_DIM
    tiles, own_tiles = length // TILE, tokens // TILE
    width_tiles = width // TILE
    dp, row, col = (lax.axis_index(name) for name in ("dp", "row", "col"))
    core, mine = lax.rem(col, 2), col // 2
    other = 1 - mine
    side = lax.rem(dp, 2)
    partner = {"dp": dp, "row": row, "col": flip(col, 1)}
    x_peer = {"dp": dp, "row": row, "col": flip(col, 2)}
    y_peer = {"dp": flip(dp, 1), "row": row, "col": col}
    dp_peers = [{"dp": flip(dp, mask), "row": row, "col": col} for mask in range(1, dp_size)]
    z_peers = [{"dp": dp, "row": flip(row, mask), "col": col} for mask in range(1, row_size)]
    z_of = [flip(row, mask) for mask in range(row_size)]
    copies = Copies(send_sem, recv_sem)
    pairs = (
        (layer_out, layer_hbm),
        (grad_inputs, inputs_hbm),
        (out_joint, joint_hbm),
        (out_inner, inner_hbm),
        (out_outer, outer_hbm),
    )
    stores = [
        pltpu.make_async_copy(src, dst, store_sem.at[i]) for i, (src, dst) in enumerate(pairs)
    ]

    def by_head(shared, kinds):
        parts = [shared]
        for i in range(heads):
            parts += [kind[:, i * HEAD_DIM : (i + 1) * HEAD_DIM] for kind in kinds]
        return jnp.concatenate(parts, axis=1)

    kinds = [query_weight[...], key_weight[...], value_weight[...]]
    own_joint[...] = by_head(output_weight[...], kinds)
    none = jnp.zeros((1, piece), F32)
    joint_bias = by_head(none, [row_of(query_bias), none, row_of(value_bias)])
    rest = jnp.zeros((6, width), F32)
    own_bias[...] = jnp.concatenate([joint_bias, row_of(inner_bias), rest], axis=0)
    barrier = pltpu.get_barrier_semaphore()
    everyone = [partner, x_peer] + dp_peers + z_peers
    for peer in everyone:
        pl.semaphore_signal(barrier, inc=1, device_id=peer, device_id_type=MESH)
    pl.semaphore_wait(barrier, len(everyone))

    own_start, far_start = core * tokens, (1 - core) * tokens

    def half_rows(z, which):
        return rows_at(z * block + which * half, half)

    def block_rows(z):
        return rows_at(z * block, block)

    class Gather:
        def __init__(self, own, full, wide):
            source = own.at[rows_at(side * half, half)]
            spot = full.at[mine, half_rows(row, side)]
            self.z = [copies.new(own, full.at[mine, block_rows(row)], z_peers[0])]
            self.z += [copies.new(source, spot, peer) for peer in z_peers[1:]]
            self.x_own = copies.new(own, full.at[mine, block_rows(row)], x_peer)
            got = [full.at[mine, half_rows(z, side)] for z in z_of[1:]]
            self.wide = 1 if wide else 0
            sent = [full.at[mine, block_rows(z_of[1])] if wide else got[0]] + got[1:]
            self.x = [copies.new(ref, ref, x_peer) for ref in sent]
            self.y = [copies.new(ref, ref, y_peer) for ref in got[1:]]
            got = [full.at[other, half_rows(z, side)] for z in z_of[1:]]
            self.xy = [copies.new(ref, ref, y_peer) for ref in got[self.wide :]]

        def start_z(self):
            for copy in self.z:
                copy.start()

        def wait_z(self):
            for copy in self.z:
                copy.wait_recv()

        def start_x(self):
            for copy in self.x[1:] + self.x[:1]:
                copy.start()

        def start_y(self):
            for copy in self.y:
                copy.start()

        def wait_y(self):
            for copy in self.y:
                copy.wait_recv()

        def across(self):
            for x, xy in zip(self.x[self.wide :], self.xy):
                x.wait_recv()
                xy.start()

        def done(self):
            self.x_own.wait_recv()
            for copy in self.x[: self.wide] + self.xy:
                copy.wait_recv()

    gathers = [
        Gather(own_joint, w_joint, False),
        Gather(own_inner, w_inner, False),
        Gather(own_outer, w_outer, True),
    ]
    gathers[0].start_z()
    gathers[0].x_own.start()
    own_rows_all = rows_at(own_start, tokens)
    send_x = copies.new(hidden, x_full.at[own_rows_all], partner)
    send_x.start()
    send_bias = copies.new(own_bias, bias_full.at[mine], x_peer)
    send_bias.start()
    for own, full in ((own_joint, w_joint), (own_inner, w_inner), (own_outer, w_outer)):
        full[mine, block_rows(row), :] = own[...]
    x_full[own_rows_all, :] = hidden[...]
    bias_full[mine] = own_bias[...]
    seg_row[...] = jnp.where(mine == 0, segments[0:1, :], segments[1:2, :]).astype(F32)
    seg_col[...] = jnp.broadcast_to(seg_row[...], (128, length)).T
    shared_sum[...] = jnp.zeros_like(shared_sum)
    bias_sum[...] = jnp.zeros_like(bias_sum)

    for index, z_copy in enumerate(gathers[0].z):
        z_copy.wait_recv()
        if index:
            gathers[0].y[index - 1].start()
        gathers[0].x[index].start()
    gathers[1].start_z()
    send_x.wait_recv()
    send_bias.wait_recv()
    gathers[0].wait_y()
    gathers[0].across()
    gathers[1].x_own.start()

    def project(h):
        def body(tile, carry):
            rows = rows_at(tile * TILE, TILE)
            out = dot(x_full[rows, :], w_joint[h, :, 128:], 1, 0) + bias_full[h, 0:1, 128:]
            for which, target in enumerate((query, keys, values)):
                for i in range(heads):
                    at = piece - 128 + (3 * i + which) * HEAD_DIM
                    part = out[:, at : at + HEAD_DIM].astype(BF16)
                    if which == 0:
                        part = part * SCALE
                    target[h * heads + i, rows, :] = part.astype(BF16)
            return carry

        lax.fori_loop(0, tiles, body, 0)

    lanes = lax.broadcasted_iota(jnp.int32, (TILE, 128), 1)
    half_steps = heads * tiles

    def at_steps(step, services):
        for when, service in services.items():

            @pl.when(step == when)
            def _(service=service):
                service()

    def forward_z():
        gathers[1].wait_z()
        gathers[1].start_y()
        gathers[1].start_x()
        gathers[2].start_z()

    def forward_across():
        gathers[1].wait_y()
        gathers[1].across()

    def forward_last():
        gathers[2].wait_z()
        gathers[2].start_x()

    before = {half_steps: gathers[0].done}
    after = {
        4: forward_z,
        half_steps - 1: gathers[2].x_own.start,
        half_steps + 2: forward_across,
        half_steps + 5: forward_last,
        half_steps + 11: gathers[2].start_y,
    }

    def attend(step, carry):
        turn = step // half_steps
        h = mine + (1 - 2 * mine) * turn
        head = h * heads + lax.rem(step, half_steps) // tiles
        tile = lax.rem(step, tiles)
        at_steps(step, before)
        pl.when(lax.rem(step, half_steps) == 0)(lambda: project(h))
        rows = rows_at(tile * TILE, TILE)
        scores = dot(query[head, rows, :], keys[head], 1, 1)
        scores = jnp.where(seg_col[rows, 0:1] == seg_row[...], scores, NEG_FILL)
        peak = jnp.max(scores, axis=1, keepdims=True)
        expos = jnp.exp(scores - peak)
        total = jnp.sum(expos, axis=1, keepdims=True)
        out = dot(expos.astype(BF16), values[head], 1, 0) / total
        head_mixed[head, rows, :] = out.astype(BF16)
        log_sums[rows, :] = jnp.where(lanes == head, peak + jnp.log(total), log_sums[rows, :])
        at_steps(step, after)
        return carry

    lax.fori_loop(0, 2 * half_steps, attend, 0)

    def join(tile, carry):
        rows = rows_at(tile * TILE, TILE)
        for h in range(2):
            parts = [head_mixed[h * heads + i, rows, :] for i in range(heads)]
            mixed[h, rows, :] = jnp.concatenate(parts, axis=1)
        return carry

    lax.fori_loop(0, tiles, join, 0)

    class Exchange:
        def __init__(self, number, partial_of):
            self.partial_of = partial_of
            self.send = send_part.at[number % 2]
            self.recv = recv_part.at[number]
            self.copies = [
                copies.new(
                    self.send.at[pl.ds(i * TILE, TILE)],
                    self.recv.at[pl.ds(i * TILE, TILE)],
                    partner,
                )
                for i in range(own_tiles)
            ]

        def give(self):
            for i, copy in enumerate(self.copies):
                part = self.partial_of(rows_at(far_start + i * TILE, TILE))
                self.send[pl.ds(i * TILE, TILE), :] = part.astype(BF16)
                copy.start()

        def take(self, i):
            part = self.partial_of(rows_at(own_start + i * TILE, TILE))
            self.copies[i].wait_recv()
            return part + self.recv[pl.ds(i * TILE, TILE), :].astype(F32)

    class Share:
        def __init__(self, full):
            self.full = full
            spots = [full.at[rows_at(own_start + i * TILE, TILE)] for i in range(own_tiles)]
            self.copies = [copies.new(ref, ref, partner) for ref in spots]

        def put(self, i, tile_rows):
            self.full[rows_at(own_start + i * TILE, TILE), :] = tile_rows
            self.copies[i].start()

        def wait(self):
            for copy in self.copies:
                copy.wait_recv()

    def mean(v):
        return jnp.sum(v, axis=1, keepdims=True) * (1.0 / width)

    def normalize(v):
        centered = v - mean(v)
        inv_scale = lax.rsqrt(mean(centered * centered) + EPS_NORM)
        return centered * inv_scale, inv_scale

    def norm_backward(grads, normed, inv_scale, gain):
        scaled = grads * gain
        return inv_scale * (scaled - mean(scaled) - normed * mean(scaled * normed))

    def add_shared(index, v):
        shared_sum[index : index + 1, :] += jnp.sum(v, axis=0, keepdims=True)

    def mixed_partial(rows):
        return dot(mixed[0, rows, :], w_joint[0, :, :piece], 1, 1) + dot(
            mixed[1, rows, :], w_joint[1, :, :piece], 1, 1
        )

    leave_one = Exchange(0, mixed_partial)
    leave_one.give()
    share_first = Share(first_rows)
    for i in range(own_tiles):
        rows = pl.ds(i * TILE, TILE)
        branch = leave_one.take(i) + row_of(output_bias)
        normed, inv_scale = normalize(hidden[rows, :].astype(F32) + branch)
        first_normed[rows, :] = normed
        first_scale[rows, :] = inv_scale
        out = normed * row_of(first_gain) + row_of(first_shift)
        share_first.put(i, out.astype(BF16))

    def inner(tile, start):
        rows = rows_at(start + tile * TILE, TILE)
        x = first_rows[rows, :]
        for h in range(2):
            pre = dot(x, w_inner[h], 1, 0) + bias_full[h, 1:2, :]
            below = 0.5 + 0.5 * lax.erf(pre * INV_SQRT2)
            density = INV_SQRT_2PI * jnp.exp(-0.5 * pre * pre)
            activated[h, rows, :] = (pre * below).astype(BF16)
            gelu_slope[h, rows, :] = (below + pre * density).astype(BF16)
        return start

    gathers[1].done()
    lax.fori_loop(0, own_tiles, inner, own_start)
    share_first.wait()
    gathers[2].wait_y()
    gathers[2].across()
    lax.fori_loop(0, own_tiles, inner, far_start)
    gathers[2].done()

    def outer_partial(rows):
        return dot(activated[0, rows, :], w_outer[0], 1, 1) + dot(
            activated[1, rows, :], w_outer[1], 1, 1
        )

    leave_two = Exchange(1, outer_partial)
    leave_two.give()
    share_two = Share(branch_two)
    for i in range(own_tiles):
        rows = pl.ds(i * TILE, TILE)
        branch = leave_two.take(i) + row_of(outer_bias)
        normed, inv_scale = normalize(
            first_normed[rows, :] * row_of(first_gain) + row_of(first_shift) + branch
        )
        layer_out[rows, :] = (normed * row_of(second_gain) + row_of(second_shift)).astype(BF16)
        grads = upstream[rows, :].astype(F32)
        back = norm_backward(grads, normed, inv_scale, row_of(second_gain))
        grad_second[rows, :] = back
        rounded = back.astype(BF16)
        share_two.put(i, rounded)
        add_shared(3, rounded.astype(F32))
        add_shared(4, grads * normed)
        add_shared(5, grads)
    share_two.wait()
    stores[0].start()

    class Reduce:
        def __init__(self, number, grads, out, lane_set):
            self.lane_set, self.out = lane_set, out.at[:, lane_set]
            self.pool, self.zr = xy_recv.at[number, :, lane_set], z_recv.at[number, :, :, lane_set]
            self.fs, self.fr = f_send.at[number, :, lane_set], f_recv.at[number, :, :, lane_set]
            self.grads = grads = grads.at[:, :, lane_set]
            away = 1 - side
            self.first, self.first_mine, self.second = [], [], []
            for j, z in enumerate(z_of):
                slot = [self.pool.at[pl.ds((3 * j + k) * half, half)] for k in range(3)]
                if j % 2 == 0:
                    both = self.pool.at[pl.ds(3 * j * half, block)]
                    self.first.append(copies.new(grads.at[other, block_rows(z)], both, x_peer))
                    self.first_mine.append(None)
                    source = grads.at[mine, half_rows(z, away)]
                    self.second.append(copies.new(source, slot[2], y_peer))
                else:
                    source = grads.at[other, half_rows(z, away)]
                    self.first.append(copies.new(source, slot[0], y_peer))
                    source = grads.at[mine, half_rows(z, away)]
                    self.first_mine.append(copies.new(source, slot[1], y_peer))
                    source = grads.at[other, half_rows(z, side)]
                    self.second.append(copies.new(source, slot[2], x_peer))
            self.third, bit = {}, 1
            while bit < row_size:
                for j in range(bit, row_size, 2 * bit):
                    source = grads.at[mine, half_rows(z_of[j], side)]
                    slot = self.zr.at[j - 1]
                    self.third[j] = copies.new(source, slot, z_peers[bit - 1])
                bit *= 2
            self.fourth = [copies.new(self.fs, self.fr.at[dp], peer) for peer in dp_peers]
            self.order = [j for j in range(row_size - 1, -1, -1) if j % 2] + [
                j for j in range(row_size - 1, -1, -1) if j % 2 == 0
            ]

        def start_other(self):
            for j in self.order:
                self.first[j].start()

        def start_mine(self):
            for j in self.order:
                if j % 2:
                    self.first_mine[j].start()

        def add(self, h, rows, *slots):
            total = self.grads[h, rows, :].astype(F32)
            for start, size in slots:
                total = total + self.pool[pl.ds(start * half, size), :].astype(F32)
            self.grads[h, rows, :] = total.astype(BF16)

        def go_second(self, odd):
            for j in self.order:
                if j % 2 == odd:
                    self.first[j].wait_recv()
                    if odd:
                        self.add(other, half_rows(z_of[j], side), (3 * j, half))
                    else:
                        self.add(mine, block_rows(z_of[j]), (3 * j, block))
                    self.second[j].start()

        def go_third(self):
            for j in self.order:
                rows = half_rows(z_of[j], side)
                if j % 2:
                    self.first_mine[j].wait_recv()
                    self.second[j].wait_recv()
                    self.add(mine, rows, (3 * j + 1, half), (3 * j + 2, half))
                else:
                    self.second[j].wait_recv()
                    self.add(mine, rows, (3 * j + 2, half))
                if j % 2:
                    self.third[j].start()

        def go_along(self):
            for j in range(2, row_size, 2):
                self.take_third(j)
                self.third[j].start()

        def take_third(self, j):
            bit = 1
            while bit < row_size and j % (2 * bit) == 0:
                self.third[j + bit].wait_recv()
                bit *= 2
            rows = half_rows(z_of[j], side)
            total = self.grads[mine, rows, :].astype(F32)
            bit = 1
            while bit < row_size and j % (2 * bit) == 0:
                total = total + self.zr[j + bit - 1].astype(F32)
                bit *= 2
            if j:
                self.grads[mine, rows, :] = total.astype(BF16)
            else:
                self.fs[...] = total.astype(BF16)

        def go_fourth(self):
            self.take_third(0)
            for copy in self.fourth:
                copy.start()

        def done(self):
            for copy in self.fourth:
                copy.wait_recv()
            self.fr[dp] = self.fs[...]
            for which in range(2):
                total = self.fr[which].astype(F32)
                for index in range(which + 2, dp_size, 2):
                    total = total + self.fr[index].astype(F32)
                self.out[pl.ds(which * half, half), :] = total

    cut = width // 2
    lane_sets = (pl.ds(0, cut), pl.ds(cut, cut))
    reduce_outer = Reduce(0, g_outer, out_outer, pl.ds(0, width))
    reduce_inner = Reduce(1, g_inner, out_inner, pl.ds(0, width))
    joint_a = Reduce(2, g_joint, out_joint, lane_sets[0])
    joint_b = Reduce(2, g_joint, out_joint, lane_sets[1])

    def weight_grad(target, rows_of, cols_of, h):
        def body(tile, carry):
            at = pl.ds(pl.multiple_of(tile * TILE, TILE), TILE)
            target[h, at, :] = dot(rows_of[:, at], cols_of[h], 0, 0).astype(BF16)
            return carry

        lax.fori_loop(0, width_tiles, body, 0)

    weight_grad(g_outer, branch_two, activated, other)
    reduce_outer.start_other()

    def back_inner(tile, carry):
        rows = rows_at(tile * TILE, TILE)
        g = branch_two[rows, :]
        for h in range(2):
            back = dot(g, w_outer[h], 1, 0) * gelu_slope[h, rows, :].astype(F32)
            rounded = back.astype(BF16)
            gelu_slope[h, rows, :] = rounded
            bias_sum[h, 1:2, :] += jnp.sum(rounded.astype(F32), axis=0, keepdims=True)
        return carry

    lax.fori_loop(0, tiles, back_inner, 0)

    def inner_back_partial(rows):
        return dot(gelu_slope[0, rows, :], w_inner[0], 1, 1) + dot(
            gelu_slope[1, rows, :], w_inner[1], 1, 1
        )

    back_one = Exchange(2, inner_back_partial)
    for copy in leave_one.copies:
        copy.wait_send()
    back_one.give()
    weight_grad(g_outer, branch_two, activated, mine)
    reduce_outer.start_mine()
    share_one = Share(branch_one)
    for i in range(own_tiles):
        rows = pl.ds(i * TILE, TILE)
        grads = back_one.take(i) + grad_second[rows, :]
        normed = first_normed[rows, :]
        back = norm_backward(grads, normed, first_scale[rows, :], row_of(first_gain))
        grad_second[rows, :] = back
        rounded = back.astype(BF16)
        share_one.put(i, rounded)
        add_shared(0, rounded.astype(F32))
        add_shared(1, grads * normed)
        add_shared(2, grads)
    send_shared = copies.new(shared_sum, shared_pair, partner)
    send_shared.start()
    weight_grad(g_inner, first_rows, gelu_slope, other)
    reduce_inner.start_other()
    weight_grad(g_inner, first_rows, gelu_slope, mine)
    reduce_inner.start_mine()
    share_one.wait()

    def back_mixed(tile, carry):
        rows = rows_at(tile * TILE, TILE)
        g = branch_one[rows, :]
        for h in range(2):
            out = dot(g, w_joint[h, :, :piece], 1, 0)
            for i in range(heads):
                part = out[:, i * HEAD_DIM : (i + 1) * HEAD_DIM]
                grad_heads[h * heads + i, rows, :] = part.astype(BF16)
        return carry

    lax.fori_loop(0, tiles, back_mixed, 0)
    reduce_outer.go_second(0)
    reduce_outer.go_second(1)

    def back_setup(head):
        q_turned[...] = query[head].T
        o_turned[...] = grad_heads[head].T
        dk_turned[...] = jnp.zeros_like(dk_turned)
        dv_turned[...] = jnp.zeros_like(dv_turned)

    def back_finish(head):
        keys[head] = dk_turned[...].T.astype(BF16)
        values[head] = dv_turned[...].T.astype(BF16)

    grad_rows = activated

    members = ([0], list(range(1, heads)))

    def gather_heads(h, which):
        lane_set = lane_sets[which]

        def body(tile, carry):
            rows = rows_at(tile * TILE, TILE)
            parts = [] if which else [jnp.zeros((TILE, piece), BF16)]
            for i in members[which]:
                parts += [source[h * heads + i, rows, :] for source in (query, keys, values)]
            joined = jnp.concatenate(parts, axis=1)
            grad_rows[h, rows, lane_set] = joined
            bias_sum[h, 0:1, lane_set] += jnp.sum(joined.astype(F32), axis=0, keepdims=True)
            return carry

        lax.fori_loop(0, tiles, body, 0)

        def joint_grad(tile, carry):
            at = pl.ds(pl.multiple_of(tile * TILE, TILE), TILE)
            g_joint[h, at, lane_set] = dot(x_full[:, at], grad_rows[h, :, lane_set], 0, 0).astype(
                BF16
            )
            if which == 0:
                g_joint[h, at, :piece] = dot(branch_one[:, at], mixed[h], 0, 0).astype(BF16)
            return carry

        lax.fori_loop(0, width_tiles, joint_grad, 0)

    after_back = {
        6: joint_a.start_other,
        8: lambda: reduce_inner.go_second(0),
        9: lambda: reduce_inner.go_second(1),
        11: lambda: (reduce_outer.go_third(), joint_b.start_other()),
        15: joint_a.start_mine,
        16: reduce_outer.go_along,
        18: lambda: joint_a.go_second(1),
        19: lambda: joint_a.go_second(0),
        20: reduce_inner.go_third,
        21: lambda: joint_b.go_second(1),
        22: reduce_outer.go_fourth,
    }

    def attend_back(step, carry):
        turn = step // half_steps
        h = other + (1 - 2 * other) * turn
        head = h * heads + lax.rem(step, half_steps) // tiles
        tile = lax.rem(step, tiles)
        pl.when(tile == 0)(lambda: back_setup(head))
        rows = rows_at(tile * TILE, TILE)
        q, g = query[head, rows, :], grad_heads[head, rows, :]
        scores = dot(q, keys[head], 1, 1)
        scores = jnp.where(seg_col[rows, 0:1] == seg_row[...], scores, NEG_FILL)
        log_sum = jnp.sum(jnp.where(lanes == head, log_sums[rows, :], 0.0), axis=1, keepdims=True)
        probs = jnp.exp(scores - log_sum)
        grad_probs = dot(g, values[head], 1, 1)
        inner_sum = jnp.sum(
            g.astype(F32) * head_mixed[head, rows, :].astype(F32), axis=1, keepdims=True
        )
        grad_scores = (probs * (grad_probs - inner_sum)).astype(BF16)
        dv_turned[...] += dot(o_turned[:, rows], probs.astype(BF16), 1, 0)
        dk_turned[...] += dot(q_turned[:, rows], grad_scores, 1, 0)
        query[head, rows, :] = (dot(grad_scores, keys[head], 1, 0) * SCALE).astype(BF16)
        pl.when(tile == tiles - 1)(lambda: back_finish(head))
        in_half = lax.rem(step, half_steps)
        pl.when(in_half == tiles - 1)(lambda: gather_heads(h, 0))
        pl.when(in_half == half_steps - 1)(lambda: gather_heads(h, 1))
        at_steps(step, after_back)
        return carry

    lax.fori_loop(0, 2 * half_steps, attend_back, 0)
    joint_b.start_mine()
    joint_b.go_second(0)
    joint_a.go_third()
    reduce_inner.go_along()

    send_shared.wait_recv()
    vec_x_send, vec_x_recv = vec_x.at[0], vec_x.at[1]
    vec_x[0, :8, :] = shared_sum[...] + shared_pair[...]
    vec_x[0, 8:, :] = bias_sum[other]
    send_vec_x = copies.new(vec_x_send, vec_x_recv, x_peer)
    send_vec_x.start()

    def input_partial(rows):
        return dot(grad_rows[0, rows, :], w_joint[0], 1, 1) + dot(
            grad_rows[1, rows, :], w_joint[1], 1, 1
        )

    back_two = Exchange(3, input_partial)
    for copy in leave_two.copies:
        copy.wait_send()
    back_two.give()
    for i in range(own_tiles):
        rows = pl.ds(i * TILE, TILE)
        grad_inputs[rows, :] = back_two.take(i) + grad_second[rows, :]
    stores[1].start()
    joint_a.go_along()
    joint_b.go_third()
    reduce_inner.go_fourth()
    reduce_outer.done()
    stores[4].start()

    send_vec_x.wait_recv()
    vec_dp[dp, :8, :] = vec_x[0, :8, :] + vec_x[1, :8, :]
    vec_dp[dp, 8:, :] = bias_sum[mine] + vec_x[1, 8:, :]
    send_vec_dp = [copies.new(vec_dp.at[dp], vec_dp.at[dp], peer) for peer in dp_peers]
    for copy in send_vec_dp:
        copy.start()
    joint_a.go_fourth()
    joint_b.go_along()
    for copy in send_vec_dp:
        copy.wait_recv()
    total = vec_dp[0]
    for index in range(1, dp_size):
        total = total + vec_dp[index]
    vec_z[row] = total
    send_vec_z = [copies.new(vec_z.at[row], vec_z.at[row], peer) for peer in z_peers]
    for copy in send_vec_z:
        copy.start()
    reduce_inner.done()
    stores[3].start()
    joint_a.done()
    joint_b.go_fourth()
    for copy in send_vec_z:
        copy.wait_recv()
    total = vec_z[0]
    for index in range(1, row_size):
        total = total + vec_z[index]
    out_shared[...] = total[:8]
    out_bias[...] = total[8:]
    joint_b.done()
    stores[2].start()
    for store in stores:
        store.wait()
    copies.finish()


def unpack_kernel(
    layer_in,
    inputs_in,
    joint_in,
    inner_in,
    outer_in,
    shared_in,
    bias_in,
    layer_out,
    inputs_out,
    query_out,
    key_out,
    value_out,
    output_out,
    inner_out,
    outer_out,
    query_bias_out,
    value_bias_out,
    *vectors_out,
):
    piece, width = query_out.shape[1], joint_in.shape[1]
    layer_out[...] = layer_in[...]
    inputs_out[...] = inputs_in[...]
    inner_out[...] = inner_in[...]
    outer_out[...] = outer_in[...]
    joint = joint_in[...]


    def of_kind(rows, which):
        starts = range(piece + which * HEAD_DIM, rows.shape[1], 3 * HEAD_DIM)
        return jnp.concatenate([rows[:, at : at + HEAD_DIM] for at in starts], axis=1)

    output_out[...] = joint[:, :piece]
    for which, out in enumerate((query_out, key_out, value_out)):
        out[...] = of_kind(joint, which)

    @pl.when(pl.program_id(0) == 0)
    def _():
        bias = bias_in[0:1, :]
        query_bias_out[...] = of_kind(bias, 0).reshape(piece)
        value_bias_out[...] = of_kind(bias, 2).reshape(piece)
        for index in range(6):
            vectors_out[index][...] = shared_in[index : index + 1, :].reshape(width)
        vectors_out[6][...] = bias_in[1:2, :].reshape(width)


def shards(
    mesh_shape,
    hidden,
    segments,
    query_weight,
    key_weight,
    value_weight,
    query_bias,
    value_bias,
    output_weight,
    output_bias,
    first_gain,
    first_shift,
    inner_weight,
    inner_bias,
    outer_weight,
    outer_bias,
    second_gain,
    second_shift,
    upstream,
):
    dp_size, row_size, col_size = mesh_shape
    tokens, width = hidden.shape
    length = segments.shape[1]
    block, piece = query_weight.shape
    hidden_units = inner_weight.shape[1]
    heads = piece // HEAD_DIM
    assert col_size == 4 and length == 2 * tokens and 4 * piece == width == hidden_units
    half = block // 2
    vmem = pl.BlockSpec(memory_space=pltpu.VMEM)

    def shape(dims, dtype):
        return jax.ShapeDtypeStruct(dims, dtype)

    per_head = pltpu.VMEM((2 * heads, length, HEAD_DIM), BF16)
    weights = pltpu.VMEM((2, width, width), BF16)
    scratch = [
        pltpu.VMEM((tokens, width), BF16),
        pltpu.VMEM((tokens, width), F32),
        pltpu.VMEM((block, width), F32),
        pltpu.VMEM((block, width), F32),
        pltpu.VMEM((block, width), F32),
        pltpu.SemaphoreType.DMA((5,)),
        pltpu.VMEM((block, width), BF16),
        pltpu.VMEM((length, 128), F32),
        pltpu.VMEM((1, length), F32),
        pltpu.VMEM((8, width), F32),
        weights,
        weights,
        weights,
        pltpu.VMEM((length, width), BF16),
        per_head,
        per_head,
        per_head,
        pltpu.VMEM((length, 128), F32),
        per_head,
        pltpu.VMEM((2, length, piece), BF16),
        pltpu.VMEM((2, 8, width), F32),
        pltpu.VMEM((tokens, width), F32),
        pltpu.VMEM((tokens, 1), F32),
        pltpu.VMEM((length, width), BF16),
        pltpu.VMEM((2, length, width), BF16),
        pltpu.VMEM((2, length, width), BF16),
        pltpu.VMEM((length, width), BF16),
        pltpu.VMEM((length, width), BF16),
        per_head,
        pltpu.VMEM((2, tokens, width), BF16),
        pltpu.VMEM((4, tokens, width), BF16),
        pltpu.VMEM((HEAD_DIM, length), BF16),
        pltpu.VMEM((HEAD_DIM, length), BF16),
        pltpu.VMEM((HEAD_DIM, length), F32),
        pltpu.VMEM((HEAD_DIM, length), F32),
        weights,
        weights,
        weights,
        pltpu.VMEM((3, 3 * width // 2, width), BF16),
        pltpu.VMEM((3, row_size - 1, half, width), BF16),
        pltpu.VMEM((3, half, width), BF16),
        pltpu.VMEM((3, dp_size, half, width), BF16),
        pltpu.VMEM((8, width), F32),
        pltpu.VMEM((2, 8, width), F32),
        pltpu.VMEM((8, width), F32),
        pltpu.VMEM((2, 16, width), F32),
        pltpu.VMEM((dp_size, 16, width), F32),
        pltpu.VMEM((row_size, 16, width), F32),
        pltpu.SemaphoreType.DMA((256,)),
        pltpu.SemaphoreType.DMA((256,)),
    ]
    results = pl.pallas_call(
        functools.partial(layer_kernel, (dp_size, row_size)),
        out_shape=[
            shape((tokens, width), BF16),
            shape((tokens, width), F32),
            shape((block, width), F32),
            shape((block, width), F32),
            shape((block, width), F32),
            shape((8, width), F32),
            shape((8, width), F32),
        ],
        in_specs=[vmem] * 18,
        out_specs=[pl.BlockSpec(memory_space=pl.ANY)] * 5 + [vmem] * 2,
        scratch_shapes=scratch,
        compiler_params=pltpu.CompilerParams(
            collective_id=0, has_side_effects=True, vmem_limit_bytes=67043328
        ),
        name="layer",
    )(
        output_weight,
        query_weight,
        key_weight,
        value_weight,
        inner_weight,
        outer_weight,
        hidden,
        upstream,
        segments,
        query_bias,
        value_bias,
        inner_bias,
        output_bias,
        first_gain,
        first_shift,
        outer_bias,
        second_gain,
        second_shift,
    )
    steps = 4

    def part(rows, columns):
        return pl.BlockSpec((rows // steps, columns), lambda i: (i, 0))

    def all_of(rows, columns):
        return pl.BlockSpec((rows, columns), lambda i: (0, 0))

    big = [part(tokens, width)] * 2
    small = [part(block, piece)] * 4
    square = [part(block, width)] * 2
    outs = pl.pallas_call(
        unpack_kernel,
        grid=(steps,),
        out_shape=[shape((tokens, width), BF16), shape((tokens, width), F32)]
        + [shape((block, piece), F32)] * 4
        + [shape((block, width), F32)] * 2
        + [shape((piece,), F32)] * 2
        + [shape((width,), F32)] * 7,
        in_specs=big + [part(block, width)] + square + [all_of(8, width)] * 2,
        out_specs=big + small + square + [pl.BlockSpec((piece,), lambda i: (0,))] * 2
        + [pl.BlockSpec((width,), lambda i: (0,))] * 7,
        name="unpack",
    )(*results)
    layer_out, grad_inputs, grad_query, grad_key, grad_value, grad_output = outs[:6]
    grad_inner, grad_outer = outs[6:8]
    vectors = outs[8:]
    return (
        layer_out,
        grad_inputs,
        grad_query,
        grad_key,
        grad_value,
        vectors[0],
        vectors[1],
        grad_output,
        vectors[2],
        vectors[3],
        vectors[4],
        grad_inner,
        vectors[8],
        grad_outer,
        vectors[5],
        vectors[6],
        vectors[7],
    )


def solution(mesh):
    tokens_spec = P(("dp", "row", "col"), None)
    weight_spec = P("row", "col")
    in_specs = (
        tokens_spec,
        P(("dp", "row"), None),
        weight_spec,
        weight_spec,
        weight_spec,
        P("col"),
        P("col"),
        weight_spec,
        P(),
        P(),
        P(),
        weight_spec,
        P("col"),
        weight_spec,
        P(),
        P(),
        P(),
        tokens_spec,
    )
    out_specs = (
        tokens_spec,
        tokens_spec,
        weight_spec,
        weight_spec,
        weight_spec,
        P("col"),
        P("col"),
        weight_spec,
        P(),
        P(),
        P(),
        weight_spec,
        P("col"),
        weight_spec,
        P(),
        P(),
        P(),
    )
    mesh_shape = (mesh.shape["dp"], mesh.shape["row"], mesh.shape["col"])
    return jax.shard_map(
        functools.partial(shards, mesh_shape),
        mesh=mesh,
        in_specs=in_specs,
        out_specs=out_specs,
        check_vma=False,
    )
```

```python
import functools

import jax
import jax.numpy as jnp
from jax import lax
from jax.experimental import pallas as pl
from jax.experimental.pallas import tpu as pltpu
from jax.sharding import PartitionSpec as P

HEAD_DIM = 64
EPS_NORM = 1e-12
NEG_FILL = -1e30
SCALE = HEAD_DIM ** (-0.5)
MESH = pl.DeviceIdType.MESH
BF16 = jnp.bfloat16
F32 = jnp.float32
TILE = 256
INV_SQRT2 = 0.7071067811865476
INV_SQRT_2PI = 0.3989422804014327


def dot(left, right, left_dim, right_dim):
    dims = (((left_dim,), (right_dim,)), ((), ()))
    return lax.dot_general(left, right, dims, preferred_element_type=F32)


def flip(index, mask):
    result, bit = index, 0
    while (1 << bit) <= mask:
        if (mask >> bit) & 1:
            result = result + (1 - 2 * lax.rem(index // (1 << bit), 2)) * (1 << bit)
        bit += 1
    return result


def row_of(ref):
    return ref[...].reshape(1, ref.shape[0])


def rows_at(start, size):
    return pl.ds(pl.multiple_of(start, 16), size)


class Copy:
    def __init__(self, descriptor):
        self.descriptor, self.started, self.sent = descriptor, False, False

    def start(self):
        self.descriptor.start()
        self.started = True

    def wait_recv(self):
        self.descriptor.wait_recv()

    def wait_send(self):
        if self.started and not self.sent:
            self.descriptor.wait_send()
            self.sent = True


class Copies:
    def __init__(self, send_sem, recv_sem):
        self.send_sem, self.recv_sem, self.made = send_sem, recv_sem, []

    def new(self, src, dst, device):
        number = len(self.made)
        copy = Copy(
            pltpu.make_async_remote_copy(
                src_ref=src,
                dst_ref=dst,
                send_sem=self.send_sem.at[number],
                recv_sem=self.recv_sem.at[number],
                device_id=device,
                device_id_type=MESH,
            )
        )
        self.made.append(copy)
        return copy

    def finish(self):
        for copy in self.made:
            copy.wait_send()


def layer_kernel(
    sizes,
    output_weight,
    query_weight,
    key_weight,
    value_weight,
    own_inner,
    own_outer,
    hidden,
    upstream,
    segments,
    query_bias,
    value_bias,
    inner_bias,
    output_bias,
    first_gain,
    first_shift,
    outer_bias,
    second_gain,
    second_shift,
    layer_hbm,
    inputs_hbm,
    joint_hbm,
    inner_hbm,
    outer_hbm,
    out_shared,
    out_bias,
    layer_out,
    grad_inputs,
    out_joint,
    out_inner,
    out_outer,
    store_sem,
    own_joint,
    seg_col,
    seg_row,
    own_bias,
    w_joint,
    w_inner,
    w_outer,
    x_full,
    query,
    keys,
    values,
    log_sums,
    head_mixed,
    mixed,
    bias_full,
    first_normed,
    first_scale,
    x_turned,
    activated,
    gelu_slope,
    branch_two,
    branch_one,
    grad_heads,
    send_part,
    recv_part,
    q_turned,
    o_turned,
    dk_turned,
    dv_turned,
    g_joint,
    g_inner,
    g_outer,
    xy_recv,
    z_recv,
    f_send,
    f_recv,
    shared_sum,
    bias_sum,
    shared_pair,
    vec_x,
    vec_dp,
    vec_z,
    send_sem,
    recv_sem,
):
    dp_size, row_size = sizes
    grad_second = grad_inputs
    first_rows = x_full
    tokens, width = hidden.shape
    length = 2 * tokens
    block = own_joint.shape[0]
    half = block // 2
    heads = w_joint.shape[2] // (4 * HEAD_DIM)
    piece = heads * HEAD_DIM
    tiles, own_tiles = length // TILE, tokens // TILE
    width_tiles = width // TILE
    dp, row, col = (lax.axis_index(name) for name in ("dp", "row", "col"))
    core, mine = lax.rem(col, 2), col // 2
    other = 1 - mine
    side = lax.rem(dp, 2)
    partner = {"dp": dp, "row": row, "col": flip(col, 1)}
    x_peer = {"dp": dp, "row": row, "col": flip(col, 2)}
    y_peer = {"dp": flip(dp, 1), "row": row, "col": col}
    dp_peers = [{"dp": flip(dp, mask), "row": row, "col": col} for mask in range(1, dp_size)]
    z_peers = [{"dp": dp, "row": flip(row, mask), "col": col} for mask in range(1, row_size)]
    z_of = [flip(row, mask) for mask in range(row_size)]
    copies = Copies(send_sem, recv_sem)
    pairs = (
        (layer_out, layer_hbm),
        (grad_inputs, inputs_hbm),
        (out_joint, joint_hbm),
        (out_inner, inner_hbm),
        (out_outer, outer_hbm),
    )
    stores = [
        pltpu.make_async_copy(src, dst, store_sem.at[i]) for i, (src, dst) in enumerate(pairs)
    ]

    def by_head(shared, kinds):
        parts = [shared]
        for i in range(heads):
            parts += [kind[:, i * HEAD_DIM : (i + 1) * HEAD_DIM] for kind in kinds]
        return jnp.concatenate(parts, axis=1)

    kinds = [query_weight[...], key_weight[...], value_weight[...]]
    own_joint[...] = by_head(output_weight[...], kinds)
    none = jnp.zeros((1, piece), F32)
    joint_bias = by_head(none, [row_of(query_bias), none, row_of(value_bias)])
    rest = jnp.zeros((6, width), F32)
    own_bias[...] = jnp.concatenate([joint_bias, row_of(inner_bias), rest], axis=0)
    barrier = pltpu.get_barrier_semaphore()
    everyone = [partner, x_peer] + dp_peers + z_peers
    for peer in everyone:
        pl.semaphore_signal(barrier, inc=1, device_id=peer, device_id_type=MESH)
    pl.semaphore_wait(barrier, len(everyone))

    own_start, far_start = core * tokens, (1 - core) * tokens

    def half_rows(z, which):
        return rows_at(z * block + which * half, half)

    def block_rows(z):
        return rows_at(z * block, block)

    class Gather:
        def __init__(self, own, full, wide):
            self.z = {}
            for j in range(1, row_size):
                bit = j & -j
                if j == 1:
                    source, spot = own, full.at[mine, block_rows(row)]
                elif j == bit:
                    source = own.at[rows_at(side * half, half)]
                    spot = full.at[mine, half_rows(row, side)]
                else:
                    source = spot = full.at[mine, half_rows(z_of[j - bit], side)]
                self.z[j] = copies.new(source, spot, z_peers[bit - 1])
            self.z_order = sorted(self.z, key=lambda j: (bin(j).count("1"), -j))
            self.x_own = copies.new(own, full.at[mine, block_rows(row)], x_peer)
            got = [full.at[mine, half_rows(z, side)] for z in z_of[1:]]
            self.wide = 1 if wide else 0
            sent = [full.at[mine, block_rows(z_of[1])] if wide else got[0]] + got[1:]
            self.x = [copies.new(ref, ref, x_peer) for ref in sent]
            self.y = [copies.new(ref, ref, y_peer) for ref in got[1:]]
            got = [full.at[other, half_rows(z, side)] for z in z_of[1:]]
            self.xy = [copies.new(ref, ref, y_peer) for ref in got[self.wide :]]

        def start_z(self):
            for j in self.z_order:
                if j & (j - 1) == 0:
                    self.z[j].start()

        def pass_z(self, j):
            self.z[j].wait_recv()
            bit = 1
            while bit < (j & -j):
                self.z[j + bit].start()
                bit *= 2

        def middle_z(self):
            for j in self.z_order:
                if j & 1 == 0:
                    self.pass_z(j)

        def wait_z(self):
            for j in self.z_order:
                if j & 1:
                    self.z[j].wait_recv()

        def start_x(self):
            for copy in self.x[1:] + self.x[:1]:
                copy.start()

        def start_y(self):
            for copy in self.y:
                copy.start()

        def wait_y(self):
            for copy in self.y:
                copy.wait_recv()

        def across(self):
            for x, xy in zip(self.x[self.wide :], self.xy):
                x.wait_recv()
                xy.start()

        def done(self):
            self.x_own.wait_recv()
            for copy in self.x[: self.wide] + self.xy:
                copy.wait_recv()

    gathers = [
        Gather(own_joint, w_joint, False),
        Gather(own_inner, w_inner, False),
        Gather(own_outer, w_outer, True),
    ]
    gathers[0].start_z()
    gathers[0].x_own.start()
    own_rows_all = rows_at(own_start, tokens)
    send_x = copies.new(hidden, x_full.at[own_rows_all], partner)
    send_x.start()
    send_bias = copies.new(own_bias, bias_full.at[mine], x_peer)
    send_bias.start()
    for own, full in ((own_joint, w_joint), (own_inner, w_inner), (own_outer, w_outer)):
        full[mine, block_rows(row), :] = own[...]
    x_full[own_rows_all, :] = hidden[...]
    bias_full[mine] = own_bias[...]
    seg_row[...] = jnp.where(mine == 0, segments[0:1, :], segments[1:2, :]).astype(F32)
    seg_col[...] = jnp.broadcast_to(seg_row[...], (128, length)).T
    shared_sum[...] = jnp.zeros_like(shared_sum)
    bias_sum[...] = jnp.zeros_like(bias_sum)

    first = gathers[0]
    for j in first.z_order:
        first.pass_z(j)
        if j > 1:
            first.y[j - 2].start()
        first.x[j - 1].start()
    gathers[1].start_z()
    send_x.wait_recv()
    send_bias.wait_recv()

    def turn(tile, carry):
        rows = pl.ds(pl.multiple_of(tile * TILE, TILE), TILE)
        x_turned[:, rows] = x_full[rows, :].T
        return carry

    lax.fori_loop(0, tiles, turn, 0)
    gathers[0].wait_y()
    gathers[0].across()
    gathers[1].x_own.start()

    def project(h):
        def body(tile, carry):
            rows = rows_at(tile * TILE, TILE)
            out = dot(x_full[rows, :], w_joint[h, :, 128:], 1, 0) + bias_full[h, 0:1, 128:]
            for which, target in enumerate((query, keys, values)):
                for i in range(heads):
                    at = piece - 128 + (3 * i + which) * HEAD_DIM
                    part = out[:, at : at + HEAD_DIM].astype(BF16)
                    if which == 0:
                        part = part * SCALE
                    target[h * heads + i, rows, :] = part.astype(BF16)
            return carry

        lax.fori_loop(0, tiles, body, 0)

    lanes = lax.broadcasted_iota(jnp.int32, (TILE, 128), 1)
    half_steps = heads * tiles

    def at_steps(step, services):
        for when, service in services.items():

            @pl.when(step == when)
            def _(service=service):
                service()

    def forward_z():
        gathers[1].wait_z()
        gathers[1].start_y()
        gathers[1].start_x()
        gathers[2].start_z()

    def forward_across():
        gathers[1].wait_y()
        gathers[1].across()

    def forward_last():
        gathers[2].wait_z()
        gathers[2].start_x()

    before = {half_steps: gathers[0].done}
    after = {
        1: gathers[1].middle_z,
        6: forward_z,
        9: gathers[2].x_own.start,
        half_steps + 1: gathers[2].middle_z,
        half_steps + 4: forward_across,
        half_steps + 7: forward_last,
        half_steps + 11: gathers[2].start_y,
    }

    def attend(step, carry):
        turn = step // half_steps
        h = mine + (1 - 2 * mine) * turn
        head = h * heads + lax.rem(step, half_steps) // tiles
        tile = lax.rem(step, tiles)
        at_steps(step, before)
        pl.when(lax.rem(step, half_steps) == 0)(lambda: project(h))
        rows = rows_at(tile * TILE, TILE)
        scores = dot(query[head, rows, :], keys[head], 1, 1)
        scores = jnp.where(seg_col[rows, 0:1] == seg_row[...], scores, NEG_FILL)
        peak = jnp.max(scores, axis=1, keepdims=True)
        expos = jnp.exp(scores - peak)
        total = jnp.sum(expos, axis=1, keepdims=True)
        out = dot(expos.astype(BF16), values[head], 1, 0) / total
        head_mixed[head, rows, :] = out.astype(BF16)
        log_sums[rows, :] = jnp.where(lanes == head, peak + jnp.log(total), log_sums[rows, :])
        at_steps(step, after)
        return carry

    lax.fori_loop(0, 2 * half_steps, attend, 0)

    def join(tile, carry):
        rows = rows_at(tile * TILE, TILE)
        for h in range(2):
            parts = [head_mixed[h * heads + i, rows, :] for i in range(heads)]
            mixed[h, rows, :] = jnp.concatenate(parts, axis=1)
        return carry

    lax.fori_loop(0, tiles, join, 0)

    class Exchange:
        def __init__(self, number, partial_of):
            self.partial_of = partial_of
            self.send = send_part.at[number % 2]
            self.recv = recv_part.at[number]
            self.copies = [
                copies.new(
                    self.send.at[pl.ds(i * TILE, TILE)],
                    self.recv.at[pl.ds(i * TILE, TILE)],
                    partner,
                )
                for i in range(own_tiles)
            ]

        def give(self):
            for i, copy in enumerate(self.copies):
                part = self.partial_of(rows_at(far_start + i * TILE, TILE))
                self.send[pl.ds(i * TILE, TILE), :] = part.astype(BF16)
                copy.start()

        def take(self, i):
            part = self.partial_of(rows_at(own_start + i * TILE, TILE))
            self.copies[i].wait_recv()
            return part + self.recv[pl.ds(i * TILE, TILE), :].astype(F32)

    class Share:
        def __init__(self, full):
            self.full = full
            spots = [full.at[rows_at(own_start + i * TILE, TILE)] for i in range(own_tiles)]
            self.copies = [copies.new(ref, ref, partner) for ref in spots]

        def put(self, i, tile_rows):
            self.full[rows_at(own_start + i * TILE, TILE), :] = tile_rows
            self.copies[i].start()

        def wait(self):
            for copy in self.copies:
                copy.wait_recv()

    def mean(v):
        return jnp.sum(v, axis=1, keepdims=True) * (1.0 / width)

    def normalize(v):
        centered = v - mean(v)
        inv_scale = lax.rsqrt(mean(centered * centered) + EPS_NORM)
        return centered * inv_scale, inv_scale

    def norm_backward(grads, normed, inv_scale, gain):
        scaled = grads * gain
        return inv_scale * (scaled - mean(scaled) - normed * mean(scaled * normed))

    def add_shared(index, v):
        shared_sum[index : index + 1, :] += jnp.sum(v, axis=0, keepdims=True)

    def mixed_partial(rows):
        return dot(mixed[0, rows, :], w_joint[0, :, :piece], 1, 1) + dot(
            mixed[1, rows, :], w_joint[1, :, :piece], 1, 1
        )

    leave_one = Exchange(0, mixed_partial)
    leave_one.give()
    share_first = Share(first_rows)
    for i in range(own_tiles):
        rows = pl.ds(i * TILE, TILE)
        branch = leave_one.take(i) + row_of(output_bias)
        normed, inv_scale = normalize(hidden[rows, :].astype(F32) + branch)
        first_normed[rows, :] = normed
        first_scale[rows, :] = inv_scale
        out = normed * row_of(first_gain) + row_of(first_shift)
        share_first.put(i, out.astype(BF16))

    def inner(tile, start):
        rows = rows_at(start + tile * TILE, TILE)
        x = first_rows[rows, :]
        for h in range(2):
            pre = dot(x, w_inner[h], 1, 0) + bias_full[h, 1:2, :]
            below = 0.5 + 0.5 * lax.erf(pre * INV_SQRT2)
            density = INV_SQRT_2PI * jnp.exp(-0.5 * pre * pre)
            activated[h, rows, :] = (pre * below).astype(BF16)
            gelu_slope[h, rows, :] = (below + pre * density).astype(BF16)
        return start

    gathers[1].done()
    lax.fori_loop(0, own_tiles, inner, own_start)
    share_first.wait()
    gathers[2].wait_y()
    gathers[2].across()
    lax.fori_loop(0, own_tiles, inner, far_start)
    gathers[2].done()

    def outer_partial(rows):
        return dot(activated[0, rows, :], w_outer[0], 1, 1) + dot(
            activated[1, rows, :], w_outer[1], 1, 1
        )

    leave_two = Exchange(1, outer_partial)
    leave_two.give()
    share_two = Share(branch_two)
    for i in range(own_tiles):
        rows = pl.ds(i * TILE, TILE)
        branch = leave_two.take(i) + row_of(outer_bias)
        normed, inv_scale = normalize(
            first_normed[rows, :] * row_of(first_gain) + row_of(first_shift) + branch
        )
        layer_out[rows, :] = (normed * row_of(second_gain) + row_of(second_shift)).astype(BF16)
        grads = upstream[rows, :].astype(F32)
        back = norm_backward(grads, normed, inv_scale, row_of(second_gain))
        grad_second[rows, :] = back
        rounded = back.astype(BF16)
        share_two.put(i, rounded)
        add_shared(3, rounded.astype(F32))
        add_shared(4, grads * normed)
        add_shared(5, grads)
    share_two.wait()
    stores[0].start()

    class Reduce:
        def __init__(self, number, grads, out, lane_set):
            self.lane_set, self.out = lane_set, out.at[:, lane_set]
            self.pool, self.zr = xy_recv.at[number, :, lane_set], z_recv.at[number, :, :, lane_set]
            self.fs, self.fr = f_send.at[number, :, lane_set], f_recv.at[number, :, :, lane_set]
            self.grads = grads = grads.at[:, :, lane_set]
            away = 1 - side
            self.first, self.first_mine, self.second = [], [], []
            for j, z in enumerate(z_of):
                slot = [self.pool.at[pl.ds((3 * j + k) * half, half)] for k in range(3)]
                if j % 2 == 0:
                    both = self.pool.at[pl.ds(3 * j * half, block)]
                    self.first.append(copies.new(grads.at[other, block_rows(z)], both, x_peer))
                    self.first_mine.append(None)
                    source = grads.at[mine, half_rows(z, away)]
                    self.second.append(copies.new(source, slot[2], y_peer))
                else:
                    source = grads.at[other, half_rows(z, away)]
                    self.first.append(copies.new(source, slot[0], y_peer))
                    source = grads.at[mine, half_rows(z, away)]
                    self.first_mine.append(copies.new(source, slot[1], y_peer))
                    source = grads.at[other, half_rows(z, side)]
                    self.second.append(copies.new(source, slot[2], x_peer))
            self.third, bit = {}, 1
            while bit < row_size:
                for j in range(bit, row_size, 2 * bit):
                    source = grads.at[mine, half_rows(z_of[j], side)]
                    slot = self.zr.at[j - 1]
                    self.third[j] = copies.new(source, slot, z_peers[bit - 1])
                bit *= 2
            self.fourth = [copies.new(self.fs, self.fr.at[dp], peer) for peer in dp_peers]
            self.order = [j for j in range(row_size - 1, -1, -1) if j % 2] + [
                j for j in range(row_size - 1, -1, -1) if j % 2 == 0
            ]

        def start_other(self):
            for j in self.order:
                self.first[j].start()

        def start_mine(self):
            for j in self.order:
                if j % 2:
                    self.first_mine[j].start()

        def add(self, h, rows, *slots):
            total = self.grads[h, rows, :].astype(F32)
            for start, size in slots:
                total = total + self.pool[pl.ds(start * half, size), :].astype(F32)
            self.grads[h, rows, :] = total.astype(BF16)

        def go_second(self, odd):
            for j in self.order:
                if j % 2 == odd:
                    self.first[j].wait_recv()
                    if odd:
                        self.add(other, half_rows(z_of[j], side), (3 * j, half))
                    else:
                        self.add(mine, block_rows(z_of[j]), (3 * j, block))
                    self.second[j].start()

        def go_third(self):
            for j in self.order:
                rows = half_rows(z_of[j], side)
                if j % 2:
                    self.first_mine[j].wait_recv()
                    self.second[j].wait_recv()
                    self.add(mine, rows, (3 * j + 1, half), (3 * j + 2, half))
                else:
                    self.second[j].wait_recv()
                    self.add(mine, rows, (3 * j + 2, half))
                if j % 2:
                    self.third[j].start()

        def go_along(self):
            for j in range(2, row_size, 2):
                self.take_third(j)
                self.third[j].start()

        def take_third(self, j):
            bit = 1
            while bit < row_size and j % (2 * bit) == 0:
                self.third[j + bit].wait_recv()
                bit *= 2
            rows = half_rows(z_of[j], side)
            total = self.grads[mine, rows, :].astype(F32)
            bit = 1
            while bit < row_size and j % (2 * bit) == 0:
                total = total + self.zr[j + bit - 1].astype(F32)
                bit *= 2
            if j:
                self.grads[mine, rows, :] = total.astype(BF16)
            else:
                self.fs[...] = total.astype(BF16)

        def go_fourth(self):
            self.take_third(0)
            for copy in self.fourth:
                copy.start()

        def done(self):
            for copy in self.fourth:
                copy.wait_recv()
            self.fr[dp] = self.fs[...]
            for which in range(2):
                total = self.fr[which].astype(F32)
                for index in range(which + 2, dp_size, 2):
                    total = total + self.fr[index].astype(F32)
                self.out[pl.ds(which * half, half), :] = total.astype(BF16)

    cut = width // 6
    lane_sets = (pl.ds(0, 3 * cut), pl.ds(3 * cut, cut), pl.ds(4 * cut, 2 * cut))
    reduce_outer = Reduce(0, g_outer, out_outer, pl.ds(0, width))
    reduce_inner = Reduce(1, g_inner, out_inner, pl.ds(0, width))
    joint_a = Reduce(2, g_joint, out_joint, lane_sets[0])
    joint_b = Reduce(2, g_joint, out_joint, lane_sets[1])
    joint_c = Reduce(2, g_joint, out_joint, lane_sets[2])

    def weight_grad(target, rows_of, cols_of, h):
        def body(tile, carry):
            at = pl.ds(pl.multiple_of(tile * TILE, TILE), TILE)
            target[h, at, :] = dot(rows_of[:, at], cols_of[h], 0, 0).astype(BF16)
            return carry

        lax.fori_loop(0, width_tiles, body, 0)

    weight_grad(g_outer, branch_two, activated, other)
    reduce_outer.start_other()

    def back_inner(tile, carry):
        rows = rows_at(tile * TILE, TILE)
        g = branch_two[rows, :]
        for h in range(2):
            back = dot(g, w_outer[h], 1, 0) * gelu_slope[h, rows, :].astype(F32)
            rounded = back.astype(BF16)
            gelu_slope[h, rows, :] = rounded
            bias_sum[h, 1:2, :] += jnp.sum(rounded.astype(F32), axis=0, keepdims=True)
        return carry

    lax.fori_loop(0, tiles, back_inner, 0)

    def inner_back_partial(rows):
        return dot(gelu_slope[0, rows, :], w_inner[0], 1, 1) + dot(
            gelu_slope[1, rows, :], w_inner[1], 1, 1
        )

    back_one = Exchange(2, inner_back_partial)
    for copy in leave_one.copies:
        copy.wait_send()
    back_one.give()
    weight_grad(g_outer, branch_two, activated, mine)
    reduce_outer.start_mine()
    share_one = Share(branch_one)
    for i in range(own_tiles):
        rows = pl.ds(i * TILE, TILE)
        grads = back_one.take(i) + grad_second[rows, :]
        normed = first_normed[rows, :]
        back = norm_backward(grads, normed, first_scale[rows, :], row_of(first_gain))
        grad_second[rows, :] = back
        rounded = back.astype(BF16)
        share_one.put(i, rounded)
        add_shared(0, rounded.astype(F32))
        add_shared(1, grads * normed)
        add_shared(2, grads)
    send_shared = copies.new(shared_sum, shared_pair, partner)
    send_shared.start()
    weight_grad(g_inner, first_rows, gelu_slope, other)
    reduce_inner.start_other()
    weight_grad(g_inner, first_rows, gelu_slope, mine)
    reduce_inner.start_mine()
    share_one.wait()

    def back_mixed(tile, carry):
        rows = rows_at(tile * TILE, TILE)
        g = branch_one[rows, :]
        for h in range(2):
            out = dot(g, w_joint[h, :, :piece], 1, 0)
            for i in range(heads):
                part = out[:, i * HEAD_DIM : (i + 1) * HEAD_DIM]
                grad_heads[h * heads + i, rows, :] = part.astype(BF16)
        return carry

    lax.fori_loop(0, tiles, back_mixed, 0)
    reduce_outer.go_second(0)
    reduce_outer.go_second(1)

    def back_setup(head):
        q_turned[...] = query[head].T
        o_turned[...] = grad_heads[head].T
        dk_turned[...] = jnp.zeros_like(dk_turned)
        dv_turned[...] = jnp.zeros_like(dv_turned)

    def back_finish(head):
        keys[head] = dk_turned[...].T.astype(BF16)
        values[head] = dv_turned[...].T.astype(BF16)

    grad_rows = activated

    kinds = (query, keys, values)
    order = [(i, kind) for i in range(heads) for kind in range(3)]
    members = (order[:3], order[3:5], order[5:])

    def gather_heads(h, which):
        lane_set = lane_sets[which]

        def body(tile, carry):
            rows = rows_at(tile * TILE, TILE)
            parts = [] if which else [jnp.zeros((TILE, piece), BF16)]
            for i, kind in members[which]:
                parts.append(kinds[kind][h * heads + i, rows, :])
            joined = jnp.concatenate(parts, axis=1)
            grad_rows[h, rows, lane_set] = joined
            bias_sum[h, 0:1, lane_set] += jnp.sum(joined.astype(F32), axis=0, keepdims=True)
            return carry

        lax.fori_loop(0, tiles, body, 0)

        def joint_grad(tile, carry):
            at = pl.ds(pl.multiple_of(tile * TILE, TILE), TILE)
            g_joint[h, at, lane_set] = dot(x_turned[at, :], grad_rows[h, :, lane_set], 1, 0).astype(
                BF16
            )
            if which == 0:
                g_joint[h, at, :piece] = dot(branch_one[:, at], mixed[h], 0, 0).astype(BF16)
            return carry

        lax.fori_loop(0, width_tiles, joint_grad, 0)

    def start_others():
        joint_b.start_other()
        joint_c.start_other()

    def second_bc():
        joint_b.go_second(1)
        joint_c.go_second(1)

    def start_middle():
        joint_b.start_mine()
        joint_b.go_second(0)

    after_back = {
        6: joint_a.start_other,
        8: lambda: reduce_inner.go_second(0),
        9: lambda: reduce_inner.go_second(1),
        11: start_others,
        12: reduce_outer.go_third,
        15: joint_a.start_mine,
        16: reduce_outer.go_along,
        17: lambda: joint_a.go_second(1),
        18: lambda: joint_a.go_second(0),
        19: start_middle,
        20: reduce_inner.go_third,
        21: second_bc,
        22: reduce_outer.go_fourth,
    }

    def attend_back(step, carry):
        turn = step // half_steps
        h = other + (1 - 2 * other) * turn
        head = h * heads + lax.rem(step, half_steps) // tiles
        tile = lax.rem(step, tiles)
        pl.when(tile == 0)(lambda: back_setup(head))
        rows = rows_at(tile * TILE, TILE)
        q, g = query[head, rows, :], grad_heads[head, rows, :]
        scores = dot(q, keys[head], 1, 1)
        scores = jnp.where(seg_col[rows, 0:1] == seg_row[...], scores, NEG_FILL)
        log_sum = jnp.sum(jnp.where(lanes == head, log_sums[rows, :], 0.0), axis=1, keepdims=True)
        probs = jnp.exp(scores - log_sum)
        grad_probs = dot(g, values[head], 1, 1)
        inner_sum = jnp.sum(
            g.astype(F32) * head_mixed[head, rows, :].astype(F32), axis=1, keepdims=True
        )
        grad_scores = (probs * (grad_probs - inner_sum)).astype(BF16)
        dv_turned[...] += dot(o_turned[:, rows], probs.astype(BF16), 1, 0)
        dk_turned[...] += dot(q_turned[:, rows], grad_scores, 1, 0)
        query[head, rows, :] = (dot(grad_scores, keys[head], 1, 0) * SCALE).astype(BF16)
        pl.when(tile == tiles - 1)(lambda: back_finish(head))
        in_half = lax.rem(step, half_steps)
        pl.when(in_half == tiles - 1)(lambda: gather_heads(h, 0))
        pl.when(in_half == 2 * tiles - 1)(lambda: gather_heads(h, 1))
        pl.when(in_half == half_steps - 1)(lambda: gather_heads(h, 2))
        at_steps(step, after_back)
        return carry

    lax.fori_loop(0, 2 * half_steps, attend_back, 0)
    joint_c.start_mine()
    joint_c.go_second(0)
    joint_a.go_third()
    reduce_inner.go_along()

    send_shared.wait_recv()
    vec_x_send, vec_x_recv = vec_x.at[0], vec_x.at[1]
    vec_x[0, :8, :] = shared_sum[...] + shared_pair[...]
    vec_x[0, 8:, :] = bias_sum[other]
    send_vec_x = copies.new(vec_x_send, vec_x_recv, x_peer)
    send_vec_x.start()

    def input_partial(rows):
        return dot(grad_rows[0, rows, :], w_joint[0], 1, 1) + dot(
            grad_rows[1, rows, :], w_joint[1], 1, 1
        )

    back_two = Exchange(3, input_partial)
    for copy in leave_two.copies:
        copy.wait_send()
    back_two.give()
    send_vec_x.wait_recv()
    vec_dp[dp, :8, :] = vec_x[0, :8, :] + vec_x[1, :8, :]
    vec_dp[dp, 8:, :] = bias_sum[mine] + vec_x[1, 8:, :]
    send_vec_dp = [copies.new(vec_dp.at[dp], vec_dp.at[dp], peer) for peer in dp_peers]
    for copy in send_vec_dp:
        copy.start()
    for i in range(own_tiles):
        rows = pl.ds(i * TILE, TILE)
        grad_inputs[rows, :] = back_two.take(i) + grad_second[rows, :]
    stores[1].start()
    joint_b.go_third()
    joint_a.go_along()
    joint_c.go_third()
    reduce_inner.go_fourth()
    reduce_outer.done()
    stores[4].start()

    for copy in send_vec_dp:
        copy.wait_recv()
    total = vec_dp[0]
    for index in range(1, dp_size):
        total = total + vec_dp[index]
    vec_z[row] = total
    send_vec_z = [copies.new(vec_z.at[row], vec_z.at[row], peer) for peer in z_peers]
    for copy in send_vec_z:
        copy.start()
    joint_b.go_along()
    joint_c.go_along()
    joint_a.go_fourth()
    reduce_inner.done()
    stores[3].start()
    joint_b.go_fourth()
    joint_c.go_fourth()
    joint_a.done()
    joint_b.done()
    for copy in send_vec_z:
        copy.wait_recv()
    total = vec_z[0]
    for index in range(1, row_size):
        total = total + vec_z[index]
    out_shared[...] = total[:8]
    out_bias[...] = total[8:]
    joint_c.done()
    stores[2].start()
    for store in stores:
        store.wait()
    copies.finish()
    assert len(copies.made) == send_sem.shape[0]


def unpack_kernel(
    layer_in,
    inputs_in,
    joint_in,
    inner_in,
    outer_in,
    shared_in,
    bias_in,
    layer_out,
    inputs_out,
    query_out,
    key_out,
    value_out,
    output_out,
    inner_out,
    outer_out,
    query_bias_out,
    value_bias_out,
    *vectors_out,
):
    piece, width = query_out.shape[1], joint_in.shape[1]
    layer_out[...] = layer_in[...]
    inputs_out[...] = inputs_in[...]
    inner_out[...] = inner_in[...].astype(F32)
    outer_out[...] = outer_in[...].astype(F32)
    joint = joint_in[...].astype(F32)


    def of_kind(rows, which):
        starts = range(piece + which * HEAD_DIM, rows.shape[1], 3 * HEAD_DIM)
        return jnp.concatenate([rows[:, at : at + HEAD_DIM] for at in starts], axis=1)

    output_out[...] = joint[:, :piece]
    for which, out in enumerate((query_out, key_out, value_out)):
        out[...] = of_kind(joint, which)

    @pl.when(pl.program_id(0) == 0)
    def _():
        bias = bias_in[0:1, :]
        query_bias_out[...] = of_kind(bias, 0).reshape(piece)
        value_bias_out[...] = of_kind(bias, 2).reshape(piece)
        for index in range(6):
            vectors_out[index][...] = shared_in[index : index + 1, :].reshape(width)
        vectors_out[6][...] = bias_in[1:2, :].reshape(width)


def shards(
    mesh_shape,
    hidden,
    segments,
    query_weight,
    key_weight,
    value_weight,
    query_bias,
    value_bias,
    output_weight,
    output_bias,
    first_gain,
    first_shift,
    inner_weight,
    inner_bias,
    outer_weight,
    outer_bias,
    second_gain,
    second_shift,
    upstream,
):
    dp_size, row_size, col_size = mesh_shape
    tokens, width = hidden.shape
    length = segments.shape[1]
    block, piece = query_weight.shape
    hidden_units = inner_weight.shape[1]
    heads = piece // HEAD_DIM
    assert col_size == 4 and length == 2 * tokens and 4 * piece == width == hidden_units
    copies_of_gather = 3 * (4 * row_size - 4) - 1
    copies_of_sums = 2 * row_size + row_size // 2 + row_size - 1 + dp_size - 1
    copies_of_vectors = 2 + dp_size - 1 + row_size - 1
    copy_count = 2 + copies_of_gather + 7 * (tokens // TILE) + 5 * copies_of_sums
    copy_count += copies_of_vectors
    half = block // 2
    vmem = pl.BlockSpec(memory_space=pltpu.VMEM)

    def shape(dims, dtype):
        return jax.ShapeDtypeStruct(dims, dtype)

    per_head = pltpu.VMEM((2 * heads, length, HEAD_DIM), BF16)
    weights = pltpu.VMEM((2, width, width), BF16)
    scratch = [
        pltpu.VMEM((tokens, width), BF16),
        pltpu.VMEM((tokens, width), F32),
        pltpu.VMEM((block, width), BF16),
        pltpu.VMEM((block, width), BF16),
        pltpu.VMEM((block, width), BF16),
        pltpu.SemaphoreType.DMA((5,)),
        pltpu.VMEM((block, width), BF16),
        pltpu.VMEM((length, 128), F32),
        pltpu.VMEM((1, length), F32),
        pltpu.VMEM((8, width), F32),
        weights,
        weights,
        weights,
        pltpu.VMEM((length, width), BF16),
        per_head,
        per_head,
        per_head,
        pltpu.VMEM((length, 128), F32),
        per_head,
        pltpu.VMEM((2, length, piece), BF16),
        pltpu.VMEM((2, 8, width), F32),
        pltpu.VMEM((tokens, width), F32),
        pltpu.VMEM((tokens, 1), F32),
        pltpu.VMEM((width, length), BF16),
        pltpu.VMEM((2, length, width), BF16),
        pltpu.VMEM((2, length, width), BF16),
        pltpu.VMEM((length, width), BF16),
        pltpu.VMEM((length, width), BF16),
        per_head,
        pltpu.VMEM((2, tokens, width), BF16),
        pltpu.VMEM((4, tokens, width), BF16),
        pltpu.VMEM((HEAD_DIM, length), BF16),
        pltpu.VMEM((HEAD_DIM, length), BF16),
        pltpu.VMEM((HEAD_DIM, length), F32),
        pltpu.VMEM((HEAD_DIM, length), F32),
        weights,
        weights,
        weights,
        pltpu.VMEM((3, 3 * width // 2, width), BF16),
        pltpu.VMEM((3, row_size - 1, half, width), BF16),
        pltpu.VMEM((3, half, width), BF16),
        pltpu.VMEM((3, dp_size, half, width), BF16),
        pltpu.VMEM((8, width), F32),
        pltpu.VMEM((2, 8, width), F32),
        pltpu.VMEM((8, width), F32),
        pltpu.VMEM((2, 16, width), F32),
        pltpu.VMEM((dp_size, 16, width), F32),
        pltpu.VMEM((row_size, 16, width), F32),
        pltpu.SemaphoreType.DMA((copy_count,)),
        pltpu.SemaphoreType.DMA((copy_count,)),
    ]
    results = pl.pallas_call(
        functools.partial(layer_kernel, (dp_size, row_size)),
        out_shape=[
            shape((tokens, width), BF16),
            shape((tokens, width), F32),
            shape((block, width), BF16),
            shape((block, width), BF16),
            shape((block, width), BF16),
            shape((8, width), F32),
            shape((8, width), F32),
        ],
        in_specs=[vmem] * 18,
        out_specs=[pl.BlockSpec(memory_space=pl.ANY)] * 5 + [vmem] * 2,
        scratch_shapes=scratch,
        compiler_params=pltpu.CompilerParams(
            collective_id=0, has_side_effects=True, vmem_limit_bytes=67043328
        ),
        name="layer",
    )(
        output_weight,
        query_weight,
        key_weight,
        value_weight,
        inner_weight,
        outer_weight,
        hidden,
        upstream,
        segments,
        query_bias,
        value_bias,
        inner_bias,
        output_bias,
        first_gain,
        first_shift,
        outer_bias,
        second_gain,
        second_shift,
    )
    steps = 2

    def part(rows, columns):
        return pl.BlockSpec((rows // steps, columns), lambda i: (i, 0))

    def all_of(rows, columns):
        return pl.BlockSpec((rows, columns), lambda i: (0, 0))

    big = [part(tokens, width)] * 2
    small = [part(block, piece)] * 4
    square = [part(block, width)] * 2
    outs = pl.pallas_call(
        unpack_kernel,
        grid=(steps,),
        out_shape=[shape((tokens, width), BF16), shape((tokens, width), F32)]
        + [shape((block, piece), F32)] * 4
        + [shape((block, width), F32)] * 2
        + [shape((piece,), F32)] * 2
        + [shape((width,), F32)] * 7,
        in_specs=big + [part(block, width)] + square + [all_of(8, width)] * 2,
        out_specs=big + small + square + [pl.BlockSpec((piece,), lambda i: (0,))] * 2
        + [pl.BlockSpec((width,), lambda i: (0,))] * 7,
        name="unpack",
    )(*results)
    layer_out, grad_inputs, grad_query, grad_key, grad_value, grad_output = outs[:6]
    grad_inner, grad_outer = outs[6:8]
    vectors = outs[8:]
    return (
        layer_out,
        grad_inputs,
        grad_query,
        grad_key,
        grad_value,
        vectors[0],
        vectors[1],
        grad_output,
        vectors[2],
        vectors[3],
        vectors[4],
        grad_inner,
        vectors[8],
        grad_outer,
        vectors[5],
        vectors[6],
        vectors[7],
    )


def solution(mesh):
    tokens_spec = P(("dp", "row", "col"), None)
    weight_spec = P("row", "col")
    in_specs = (
        tokens_spec,
        P(("dp", "row"), None),
        weight_spec,
        weight_spec,
        weight_spec,
        P("col"),
        P("col"),
        weight_spec,
        P(),
        P(),
        P(),
        weight_spec,
        P("col"),
        weight_spec,
        P(),
        P(),
        P(),
        tokens_spec,
    )
    out_specs = (
        tokens_spec,
        tokens_spec,
        weight_spec,
        weight_spec,
        weight_spec,
        P("col"),
        P("col"),
        weight_spec,
        P(),
        P(),
        P(),
        weight_spec,
        P("col"),
        weight_spec,
        P(),
        P(),
        P(),
    )
    mesh_shape = (mesh.shape["dp"], mesh.shape["row"], mesh.shape["col"])
    return jax.shard_map(
        functools.partial(shards, mesh_shape),
        mesh=mesh,
        in_specs=in_specs,
        out_specs=out_specs,
        check_vma=False,
    )
```

```python
import functools

import jax
import jax.numpy as jnp
from jax import lax
from jax.experimental import pallas as pl
from jax.experimental.pallas import tpu as pltpu
from jax.sharding import PartitionSpec as P

HEAD_DIM = 64
EPS_NORM = 1e-12
NEG_FILL = -1e30
SCALE = HEAD_DIM ** (-0.5)
MESH = pl.DeviceIdType.MESH
BF16 = jnp.bfloat16
F32 = jnp.float32
TILE = 256
INV_SQRT2 = 0.7071067811865476
INV_SQRT_2PI = 0.3989422804014327


def dot(left, right, left_dim, right_dim):
    dims = (((left_dim,), (right_dim,)), ((), ()))
    return lax.dot_general(left, right, dims, preferred_element_type=F32)


def flip(index, mask):
    result, bit = index, 0
    while (1 << bit) <= mask:
        if (mask >> bit) & 1:
            result = result + (1 - 2 * lax.rem(index // (1 << bit), 2)) * (1 << bit)
        bit += 1
    return result


def row_of(ref):
    return ref[...].reshape(1, ref.shape[0])


def rows_at(start, size):
    return pl.ds(pl.multiple_of(start, 16), size)


class Copy:
    def __init__(self, descriptor):
        self.descriptor, self.started, self.sent = descriptor, False, False

    def start(self):
        self.descriptor.start()
        self.started = True

    def wait_recv(self):
        self.descriptor.wait_recv()

    def wait_send(self):
        if self.started and not self.sent:
            self.descriptor.wait_send()
            self.sent = True


class Copies:
    def __init__(self, send_sem, recv_sem):
        self.send_sem, self.recv_sem, self.made = send_sem, recv_sem, []

    def new(self, src, dst, device):
        number = len(self.made)
        copy = Copy(
            pltpu.make_async_remote_copy(
                src_ref=src,
                dst_ref=dst,
                send_sem=self.send_sem.at[number],
                recv_sem=self.recv_sem.at[number],
                device_id=device,
                device_id_type=MESH,
            )
        )
        self.made.append(copy)
        return copy

    def finish(self):
        for copy in self.made:
            copy.wait_send()


def layer_kernel(
    sizes,
    output_weight,
    query_weight,
    key_weight,
    value_weight,
    own_inner,
    own_outer,
    hidden,
    upstream,
    segments,
    query_bias,
    value_bias,
    inner_bias,
    output_bias,
    first_gain,
    first_shift,
    outer_bias,
    second_gain,
    second_shift,
    layer_hbm,
    inputs_hbm,
    joint_hbm,
    inner_hbm,
    outer_hbm,
    out_shared,
    out_bias,
    layer_out,
    grad_inputs,
    out_joint,
    out_inner,
    out_outer,
    store_sem,
    own_joint,
    seg_col,
    seg_row,
    own_bias,
    w_joint,
    w_inner,
    w_outer,
    x_full,
    query,
    keys,
    values,
    log_sums,
    head_mixed,
    mixed,
    bias_full,
    first_normed,
    first_scale,
    x_turned,
    activated,
    gelu_slope,
    branch_two,
    branch_one,
    grad_heads,
    send_part,
    recv_part,
    q_turned,
    o_turned,
    dk_turned,
    dv_turned,
    g_joint,
    g_inner,
    g_outer,
    xy_recv,
    z_recv,
    f_send,
    f_recv,
    shared_sum,
    bias_sum,
    shared_pair,
    vec_x,
    vec_dp,
    vec_z,
    send_sem,
    recv_sem,
):
    dp_size, row_size = sizes
    grad_second = grad_inputs
    first_rows = x_full
    tokens, width = hidden.shape
    length = 2 * tokens
    block = own_joint.shape[0]
    half = block // 2
    heads = w_joint.shape[2] // (4 * HEAD_DIM)
    piece = heads * HEAD_DIM
    tiles, own_tiles = length // TILE, tokens // TILE
    width_tiles = width // TILE
    dp, row, col = (lax.axis_index(name) for name in ("dp", "row", "col"))
    core, mine = lax.rem(col, 2), col // 2
    other = 1 - mine
    side = lax.rem(dp, 2)
    partner = {"dp": dp, "row": row, "col": flip(col, 1)}
    x_peer = {"dp": dp, "row": row, "col": flip(col, 2)}
    y_peer = {"dp": flip(dp, 1), "row": row, "col": col}
    dp_peers = [{"dp": flip(dp, mask), "row": row, "col": col} for mask in range(1, dp_size)]
    z_peers = [{"dp": dp, "row": flip(row, mask), "col": col} for mask in range(1, row_size)]
    z_of = [flip(row, mask) for mask in range(row_size)]
    copies = Copies(send_sem, recv_sem)
    pairs = (
        (layer_out, layer_hbm),
        (grad_inputs, inputs_hbm),
        (out_joint, joint_hbm),
        (out_inner, inner_hbm),
        (out_outer, outer_hbm),
    )
    stores = [
        pltpu.make_async_copy(src, dst, store_sem.at[i]) for i, (src, dst) in enumerate(pairs)
    ]

    def by_head(shared, kinds):
        parts = [shared]
        for i in range(heads):
            parts += [kind[:, i * HEAD_DIM : (i + 1) * HEAD_DIM] for kind in kinds]
        return jnp.concatenate(parts, axis=1)

    kinds = [query_weight[...], key_weight[...], value_weight[...]]
    own_joint[...] = by_head(output_weight[...], kinds)
    none = jnp.zeros((1, piece), F32)
    joint_bias = by_head(none, [row_of(query_bias), none, row_of(value_bias)])
    rest = jnp.zeros((6, width), F32)
    own_bias[...] = jnp.concatenate([joint_bias, row_of(inner_bias), rest], axis=0)
    barrier = pltpu.get_barrier_semaphore()
    everyone = [partner, x_peer] + dp_peers + z_peers
    for peer in everyone:
        pl.semaphore_signal(barrier, inc=1, device_id=peer, device_id_type=MESH)
    pl.semaphore_wait(barrier, len(everyone))

    own_start, far_start = core * tokens, (1 - core) * tokens

    def half_rows(z, which):
        return rows_at(z * block + which * half, half)

    def block_rows(z):
        return rows_at(z * block, block)

    class Gather:
        def __init__(self, own, full, wide):
            self.z = {}
            for j in range(1, row_size):
                bit = j & -j
                if j == 1:
                    source, spot = own, full.at[mine, block_rows(row)]
                elif j == bit:
                    source = own.at[rows_at(side * half, half)]
                    spot = full.at[mine, half_rows(row, side)]
                else:
                    source = spot = full.at[mine, half_rows(z_of[j - bit], side)]
                self.z[j] = copies.new(source, spot, z_peers[bit - 1])
            self.z_order = sorted(self.z, key=lambda j: (bin(j).count("1"), -j))
            self.x_own = copies.new(own, full.at[mine, block_rows(row)], x_peer)
            got = [full.at[mine, half_rows(z, side)] for z in z_of[1:]]
            self.wide = 1 if wide else 0
            sent = [full.at[mine, block_rows(z_of[1])] if wide else got[0]] + got[1:]
            self.x = [copies.new(ref, ref, x_peer) for ref in sent]
            self.y = [copies.new(ref, ref, y_peer) for ref in got[1:]]
            got = [full.at[other, half_rows(z, side)] for z in z_of[1:]]
            self.xy = [copies.new(ref, ref, y_peer) for ref in got[self.wide :]]

        def start_z(self):
            for j in self.z_order:
                if j & (j - 1) == 0:
                    self.z[j].start()

        def pass_z(self, j):
            self.z[j].wait_recv()
            bit = 1
            while bit < (j & -j):
                self.z[j + bit].start()
                bit *= 2

        def middle_z(self):
            for j in self.z_order:
                if j & 1 == 0:
                    self.pass_z(j)

        def wait_z(self):
            for j in self.z_order:
                if j & 1:
                    self.z[j].wait_recv()

        def start_x(self):
            for copy in self.x[1:] + self.x[:1]:
                copy.start()

        def start_y(self):
            for copy in self.y:
                copy.start()

        def wait_y(self):
            for copy in self.y:
                copy.wait_recv()

        def across(self):
            for x, xy in zip(self.x[self.wide :], self.xy):
                x.wait_recv()
                xy.start()

        def done(self):
            self.x_own.wait_recv()
            for copy in self.x[: self.wide] + self.xy:
                copy.wait_recv()

    gathers = [
        Gather(own_joint, w_joint, False),
        Gather(own_inner, w_inner, False),
        Gather(own_outer, w_outer, True),
    ]
    gathers[0].start_z()
    gathers[0].x_own.start()
    own_rows_all = rows_at(own_start, tokens)
    send_x = copies.new(hidden, x_full.at[own_rows_all], partner)
    send_x.start()
    send_bias = copies.new(own_bias, bias_full.at[mine], x_peer)
    send_bias.start()
    for own, full in ((own_joint, w_joint), (own_inner, w_inner), (own_outer, w_outer)):
        full[mine, block_rows(row), :] = own[...]
    x_full[own_rows_all, :] = hidden[...]
    bias_full[mine] = own_bias[...]
    seg_row[...] = jnp.where(mine == 0, segments[0:1, :], segments[1:2, :]).astype(F32)
    seg_col[...] = jnp.broadcast_to(seg_row[...], (128, length)).T
    shared_sum[...] = jnp.zeros_like(shared_sum)
    bias_sum[...] = jnp.zeros_like(bias_sum)

    first = gathers[0]
    for j in first.z_order:
        first.pass_z(j)
        if j > 1:
            first.y[j - 2].start()
        first.x[j - 1].start()
    gathers[1].start_z()
    send_x.wait_recv()
    send_bias.wait_recv()

    def turn(tile, carry):
        rows = pl.ds(pl.multiple_of(tile * TILE, TILE), TILE)
        x_turned[:, rows] = x_full[rows, :].T
        return carry

    lax.fori_loop(0, tiles, turn, 0)
    gathers[0].wait_y()
    gathers[0].across()
    gathers[1].x_own.start()

    def project(h):
        def body(tile, carry):
            rows = rows_at(tile * TILE, TILE)
            out = dot(x_full[rows, :], w_joint[h, :, 128:], 1, 0) + bias_full[h, 0:1, 128:]
            for which, target in enumerate((query, keys, values)):
                for i in range(heads):
                    at = piece - 128 + (3 * i + which) * HEAD_DIM
                    part = out[:, at : at + HEAD_DIM].astype(BF16)
                    if which == 0:
                        part = part * SCALE
                    target[h * heads + i, rows, :] = part.astype(BF16)
            return carry

        lax.fori_loop(0, tiles, body, 0)

    lanes = lax.broadcasted_iota(jnp.int32, (TILE, 128), 1)
    half_steps = heads * tiles

    def at_steps(step, services):
        for when, service in services.items():

            @pl.when(step == when)
            def _(service=service):
                service()

    def forward_z():
        gathers[1].wait_z()
        gathers[1].start_y()
        gathers[1].start_x()
        gathers[2].start_z()

    def forward_across():
        gathers[1].wait_y()
        gathers[1].across()

    def forward_last():
        gathers[2].wait_z()
        gathers[2].start_x()

    before = {half_steps: gathers[0].done}
    after = {
        1: gathers[1].middle_z,
        6: forward_z,
        half_steps + 1: gathers[2].middle_z,
        half_steps + 3: forward_across,
        half_steps + 4: gathers[2].x_own.start,
        half_steps + 7: forward_last,
        half_steps + 11: gathers[2].start_y,
    }

    def attend(step, carry):
        turn = step // half_steps
        h = mine + (1 - 2 * mine) * turn
        head = h * heads + lax.rem(step, half_steps) // tiles
        tile = lax.rem(step, tiles)
        at_steps(step, before)
        pl.when(lax.rem(step, half_steps) == 0)(lambda: project(h))
        rows = rows_at(tile * TILE, TILE)
        scores = dot(query[head, rows, :], keys[head], 1, 1)
        scores = jnp.where(seg_col[rows, 0:1] == seg_row[...], scores, NEG_FILL)
        peak = jnp.max(scores, axis=1, keepdims=True)
        expos = jnp.exp(scores - peak)
        total = jnp.sum(expos, axis=1, keepdims=True)
        out = dot(expos.astype(BF16), values[head], 1, 0) / total
        head_mixed[head, rows, :] = out.astype(BF16)
        log_sums[rows, :] = jnp.where(lanes == head, peak + jnp.log(total), log_sums[rows, :])
        at_steps(step, after)
        return carry

    lax.fori_loop(0, 2 * half_steps, attend, 0)

    def join(tile, carry):
        rows = rows_at(tile * TILE, TILE)
        for h in range(2):
            parts = [head_mixed[h * heads + i, rows, :] for i in range(heads)]
            mixed[h, rows, :] = jnp.concatenate(parts, axis=1)
        return carry

    lax.fori_loop(0, tiles, join, 0)

    class Exchange:
        def __init__(self, number, partial_of):
            self.partial_of = partial_of
            self.send = send_part.at[number % 2]
            self.recv = recv_part.at[number]
            self.copies = [
                copies.new(
                    self.send.at[pl.ds(i * TILE, TILE)],
                    self.recv.at[pl.ds(i * TILE, TILE)],
                    partner,
                )
                for i in range(own_tiles)
            ]

        def give(self):
            for i, copy in enumerate(self.copies):
                part = self.partial_of(rows_at(far_start + i * TILE, TILE))
                self.send[pl.ds(i * TILE, TILE), :] = part.astype(BF16)
                copy.start()

        def take(self, i):
            part = self.partial_of(rows_at(own_start + i * TILE, TILE))
            self.copies[i].wait_recv()
            return part + self.recv[pl.ds(i * TILE, TILE), :].astype(F32)

    class Share:
        def __init__(self, full):
            self.full = full
            spots = [full.at[rows_at(own_start + i * TILE, TILE)] for i in range(own_tiles)]
            self.copies = [copies.new(ref, ref, partner) for ref in spots]

        def put(self, i, tile_rows):
            self.full[rows_at(own_start + i * TILE, TILE), :] = tile_rows
            self.copies[i].start()

        def wait(self):
            for copy in self.copies:
                copy.wait_recv()

    def mean(v):
        return jnp.sum(v, axis=1, keepdims=True) * (1.0 / width)

    def normalize(v):
        centered = v - mean(v)
        inv_scale = lax.rsqrt(mean(centered * centered) + EPS_NORM)
        return centered * inv_scale, inv_scale

    def norm_backward(grads, normed, inv_scale, gain):
        scaled = grads * gain
        return inv_scale * (scaled - mean(scaled) - normed * mean(scaled * normed))

    def add_shared(index, v):
        shared_sum[index : index + 1, :] += jnp.sum(v, axis=0, keepdims=True)

    def mixed_partial(rows):
        return dot(mixed[0, rows, :], w_joint[0, :, :piece], 1, 1) + dot(
            mixed[1, rows, :], w_joint[1, :, :piece], 1, 1
        )

    leave_one = Exchange(0, mixed_partial)
    leave_one.give()
    share_first = Share(first_rows)
    for i in range(own_tiles):
        rows = pl.ds(i * TILE, TILE)
        branch = leave_one.take(i) + row_of(output_bias)
        normed, inv_scale = normalize(hidden[rows, :].astype(F32) + branch)
        first_normed[rows, :] = normed
        first_scale[rows, :] = inv_scale
        out = normed * row_of(first_gain) + row_of(first_shift)
        share_first.put(i, out.astype(BF16))

    def inner(tile, start):
        rows = rows_at(start + tile * TILE, TILE)
        x = first_rows[rows, :]
        for h in range(2):
            pre = dot(x, w_inner[h], 1, 0) + bias_full[h, 1:2, :]
            below = 0.5 + 0.5 * lax.erf(pre * INV_SQRT2)
            density = INV_SQRT_2PI * jnp.exp(-0.5 * pre * pre)
            activated[h, rows, :] = (pre * below).astype(BF16)
            gelu_slope[h, rows, :] = (below + pre * density).astype(BF16)
        return start

    gathers[1].done()
    lax.fori_loop(0, own_tiles, inner, own_start)
    share_first.wait()
    gathers[2].wait_y()
    gathers[2].across()
    lax.fori_loop(0, own_tiles, inner, far_start)
    gathers[2].done()

    def outer_partial(rows):
        return dot(activated[0, rows, :], w_outer[0], 1, 1) + dot(
            activated[1, rows, :], w_outer[1], 1, 1
        )

    leave_two = Exchange(1, outer_partial)
    leave_two.give()
    share_two = Share(branch_two)
    for i in range(own_tiles):
        rows = pl.ds(i * TILE, TILE)
        branch = leave_two.take(i) + row_of(outer_bias)
        normed, inv_scale = normalize(
            first_normed[rows, :] * row_of(first_gain) + row_of(first_shift) + branch
        )
        layer_out[rows, :] = (normed * row_of(second_gain) + row_of(second_shift)).astype(BF16)
        grads = upstream[rows, :].astype(F32)
        back = norm_backward(grads, normed, inv_scale, row_of(second_gain))
        grad_second[rows, :] = back
        rounded = back.astype(BF16)
        share_two.put(i, rounded)
        add_shared(3, rounded.astype(F32))
        add_shared(4, grads * normed)
        add_shared(5, grads)
    share_two.wait()
    stores[0].start()

    class Reduce:
        def __init__(self, number, grads, out, lane_set):
            self.lane_set, self.out = lane_set, out.at[:, lane_set]
            self.pool, self.zr = xy_recv.at[number, :, lane_set], z_recv.at[number, :, :, lane_set]
            self.fs, self.fr = f_send.at[number, :, lane_set], f_recv.at[number, :, :, lane_set]
            self.grads = grads = grads.at[:, :, lane_set]
            away = 1 - side
            self.first, self.first_mine, self.second = [], [], []
            for j, z in enumerate(z_of):
                slot = [self.pool.at[pl.ds((3 * j + k) * half, half)] for k in range(3)]
                if j % 2 == 0:
                    both = self.pool.at[pl.ds(3 * j * half, block)]
                    self.first.append(copies.new(grads.at[other, block_rows(z)], both, x_peer))
                    self.first_mine.append(None)
                    source = grads.at[mine, half_rows(z, away)]
                    self.second.append(copies.new(source, slot[2], y_peer))
                else:
                    source = grads.at[other, half_rows(z, away)]
                    self.first.append(copies.new(source, slot[0], y_peer))
                    source = grads.at[mine, half_rows(z, away)]
                    self.first_mine.append(copies.new(source, slot[1], y_peer))
                    source = grads.at[other, half_rows(z, side)]
                    self.second.append(copies.new(source, slot[2], x_peer))
            self.third, bit = {}, 1
            while bit < row_size:
                for j in range(bit, row_size, 2 * bit):
                    source = grads.at[mine, half_rows(z_of[j], side)]
                    slot = self.zr.at[j - 1]
                    self.third[j] = copies.new(source, slot, z_peers[bit - 1])
                bit *= 2
            self.fourth = [copies.new(self.fs, self.fr.at[dp], peer) for peer in dp_peers]
            self.order = [j for j in range(row_size - 1, -1, -1) if j % 2] + [
                j for j in range(row_size - 1, -1, -1) if j % 2 == 0
            ]

        def start_other(self):
            for j in self.order:
                self.first[j].start()

        def start_mine(self):
            for j in self.order:
                if j % 2:
                    self.first_mine[j].start()

        def add(self, h, rows, *slots):
            total = self.grads[h, rows, :].astype(F32)
            for start, size in slots:
                total = total + self.pool[pl.ds(start * half, size), :].astype(F32)
            self.grads[h, rows, :] = total.astype(BF16)

        def go_second(self, odd):
            for j in self.order:
                if j % 2 == odd:
                    self.first[j].wait_recv()
                    if odd:
                        self.add(other, half_rows(z_of[j], side), (3 * j, half))
                    else:
                        self.add(mine, block_rows(z_of[j]), (3 * j, block))
                    self.second[j].start()

        def go_third(self):
            for j in self.order:
                rows = half_rows(z_of[j], side)
                if j % 2:
                    self.first_mine[j].wait_recv()
                    self.second[j].wait_recv()
                    self.add(mine, rows, (3 * j + 1, half), (3 * j + 2, half))
                else:
                    self.second[j].wait_recv()
                    self.add(mine, rows, (3 * j + 2, half))
                if j % 2:
                    self.third[j].start()

        def go_along(self):
            for j in range(2, row_size, 2):
                self.take_third(j)
                self.third[j].start()

        def take_third(self, j):
            bit = 1
            while bit < row_size and j % (2 * bit) == 0:
                self.third[j + bit].wait_recv()
                bit *= 2
            rows = half_rows(z_of[j], side)
            total = self.grads[mine, rows, :].astype(F32)
            bit = 1
            while bit < row_size and j % (2 * bit) == 0:
                total = total + self.zr[j + bit - 1].astype(F32)
                bit *= 2
            if j:
                self.grads[mine, rows, :] = total.astype(BF16)
            else:
                self.fs[...] = total.astype(BF16)

        def go_fourth(self):
            self.take_third(0)
            for copy in self.fourth:
                copy.start()

        def done(self):
            for copy in self.fourth:
                copy.wait_recv()
            self.fr[dp] = self.fs[...]
            for which in range(2):
                total = self.fr[which].astype(F32)
                for index in range(which + 2, dp_size, 2):
                    total = total + self.fr[index].astype(F32)
                self.out[pl.ds(which * half, half), :] = total.astype(BF16)

    cut = width // 6
    lane_sets = (pl.ds(0, 3 * cut), pl.ds(3 * cut, cut), pl.ds(4 * cut, 2 * cut))
    reduce_outer = Reduce(0, g_outer, out_outer, pl.ds(0, width))
    reduce_inner = Reduce(1, g_inner, out_inner, pl.ds(0, width))
    joint_a = Reduce(2, g_joint, out_joint, lane_sets[0])
    joint_b = Reduce(2, g_joint, out_joint, lane_sets[1])
    joint_c = Reduce(2, g_joint, out_joint, lane_sets[2])

    def weight_grad(target, rows_of, cols_of, h):
        def body(tile, carry):
            at = pl.ds(pl.multiple_of(tile * TILE, TILE), TILE)
            target[h, at, :] = dot(rows_of[:, at], cols_of[h], 0, 0).astype(BF16)
            return carry

        lax.fori_loop(0, width_tiles, body, 0)

    weight_grad(g_outer, branch_two, activated, other)
    reduce_outer.start_other()

    def back_inner(tile, carry):
        rows = rows_at(tile * TILE, TILE)
        g = branch_two[rows, :]
        for h in range(2):
            back = dot(g, w_outer[h], 1, 0) * gelu_slope[h, rows, :].astype(F32)
            rounded = back.astype(BF16)
            gelu_slope[h, rows, :] = rounded
            bias_sum[h, 1:2, :] += jnp.sum(rounded.astype(F32), axis=0, keepdims=True)
        return carry

    lax.fori_loop(0, tiles, back_inner, 0)

    def inner_back_partial(rows):
        return dot(gelu_slope[0, rows, :], w_inner[0], 1, 1) + dot(
            gelu_slope[1, rows, :], w_inner[1], 1, 1
        )

    back_one = Exchange(2, inner_back_partial)
    for copy in leave_one.copies:
        copy.wait_send()
    back_one.give()
    weight_grad(g_outer, branch_two, activated, mine)
    reduce_outer.start_mine()
    share_one = Share(branch_one)
    for i in range(own_tiles):
        rows = pl.ds(i * TILE, TILE)
        grads = back_one.take(i) + grad_second[rows, :]
        normed = first_normed[rows, :]
        back = norm_backward(grads, normed, first_scale[rows, :], row_of(first_gain))
        grad_second[rows, :] = back
        rounded = back.astype(BF16)
        share_one.put(i, rounded)
        add_shared(0, rounded.astype(F32))
        add_shared(1, grads * normed)
        add_shared(2, grads)
    send_shared = copies.new(shared_sum, shared_pair, partner)
    send_shared.start()
    weight_grad(g_inner, first_rows, gelu_slope, other)
    reduce_inner.start_other()
    weight_grad(g_inner, first_rows, gelu_slope, mine)
    reduce_inner.start_mine()
    share_one.wait()

    def back_mixed(tile, carry):
        rows = rows_at(tile * TILE, TILE)
        g = branch_one[rows, :]
        for h in range(2):
            out = dot(g, w_joint[h, :, :piece], 1, 0)
            for i in range(heads):
                part = out[:, i * HEAD_DIM : (i + 1) * HEAD_DIM]
                grad_heads[h * heads + i, rows, :] = part.astype(BF16)
        return carry

    lax.fori_loop(0, tiles, back_mixed, 0)
    reduce_outer.go_second(0)
    reduce_outer.go_second(1)

    def back_setup(head):
        q_turned[...] = query[head].T
        o_turned[...] = grad_heads[head].T
        dk_turned[...] = jnp.zeros_like(dk_turned)
        dv_turned[...] = jnp.zeros_like(dv_turned)

    def back_finish(head):
        keys[head] = dk_turned[...].T.astype(BF16)
        values[head] = dv_turned[...].T.astype(BF16)

    grad_rows = activated

    kinds = (query, keys, values)
    order = [(i, kind) for i in range(heads) for kind in range(3)]
    members = (order[:3], order[3:5], order[5:])

    def gather_heads(h, which):
        lane_set = lane_sets[which]

        def body(tile, carry):
            rows = rows_at(tile * TILE, TILE)
            parts = [] if which else [jnp.zeros((TILE, piece), BF16)]
            for i, kind in members[which]:
                parts.append(kinds[kind][h * heads + i, rows, :])
            joined = jnp.concatenate(parts, axis=1)
            grad_rows[h, rows, lane_set] = joined
            bias_sum[h, 0:1, lane_set] += jnp.sum(joined.astype(F32), axis=0, keepdims=True)
            return carry

        lax.fori_loop(0, tiles, body, 0)

        def joint_grad(tile, carry):
            at = pl.ds(pl.multiple_of(tile * TILE, TILE), TILE)
            g_joint[h, at, lane_set] = dot(x_turned[at, :], grad_rows[h, :, lane_set], 1, 0).astype(
                BF16
            )
            if which == 0:
                g_joint[h, at, :piece] = dot(branch_one[:, at], mixed[h], 0, 0).astype(BF16)
            return carry

        lax.fori_loop(0, width_tiles, joint_grad, 0)

    def start_others():
        joint_b.start_other()
        joint_c.start_other()

    def second_bc():
        joint_b.go_second(1)
        joint_c.go_second(1)

    def start_middle():
        joint_b.start_mine()
        joint_b.go_second(0)

    after_back = {
        6: joint_a.start_other,
        8: lambda: reduce_inner.go_second(0),
        9: lambda: reduce_inner.go_second(1),
        11: start_others,
        12: reduce_outer.go_third,
        15: joint_a.start_mine,
        16: reduce_outer.go_along,
        17: lambda: joint_a.go_second(1),
        18: lambda: joint_a.go_second(0),
        19: start_middle,
        20: reduce_inner.go_third,
        21: second_bc,
        22: reduce_outer.go_fourth,
    }

    def attend_back(step, carry):
        turn = step // half_steps
        h = other + (1 - 2 * other) * turn
        head = h * heads + lax.rem(step, half_steps) // tiles
        tile = lax.rem(step, tiles)
        pl.when(tile == 0)(lambda: back_setup(head))
        rows = rows_at(tile * TILE, TILE)
        q, g = query[head, rows, :], grad_heads[head, rows, :]
        scores = dot(q, keys[head], 1, 1)
        scores = jnp.where(seg_col[rows, 0:1] == seg_row[...], scores, NEG_FILL)
        log_sum = jnp.sum(jnp.where(lanes == head, log_sums[rows, :], 0.0), axis=1, keepdims=True)
        probs = jnp.exp(scores - log_sum)
        grad_probs = dot(g, values[head], 1, 1)
        inner_sum = jnp.sum(
            g.astype(F32) * head_mixed[head, rows, :].astype(F32), axis=1, keepdims=True
        )
        grad_scores = (probs * (grad_probs - inner_sum)).astype(BF16)
        dv_turned[...] += dot(o_turned[:, rows], probs.astype(BF16), 1, 0)
        dk_turned[...] += dot(q_turned[:, rows], grad_scores, 1, 0)
        query[head, rows, :] = (dot(grad_scores, keys[head], 1, 0) * SCALE).astype(BF16)
        pl.when(tile == tiles - 1)(lambda: back_finish(head))
        in_half = lax.rem(step, half_steps)
        pl.when(in_half == tiles - 1)(lambda: gather_heads(h, 0))
        pl.when(in_half == 2 * tiles - 1)(lambda: gather_heads(h, 1))
        pl.when(in_half == half_steps - 1)(lambda: gather_heads(h, 2))
        at_steps(step, after_back)
        return carry

    lax.fori_loop(0, 2 * half_steps, attend_back, 0)
    joint_c.start_mine()
    joint_c.go_second(0)
    joint_a.go_third()
    reduce_inner.go_along()

    send_shared.wait_recv()
    vec_x_send, vec_x_recv = vec_x.at[0], vec_x.at[1]
    vec_x[0, :8, :] = shared_sum[...] + shared_pair[...]
    vec_x[0, 8:, :] = bias_sum[other]
    send_vec_x = copies.new(vec_x_send, vec_x_recv, x_peer)
    send_vec_x.start()

    def input_partial(rows):
        return dot(grad_rows[0, rows, :], w_joint[0], 1, 1) + dot(
            grad_rows[1, rows, :], w_joint[1], 1, 1
        )

    back_two = Exchange(3, input_partial)
    for copy in leave_two.copies:
        copy.wait_send()
    back_two.give()
    send_vec_x.wait_recv()
    vec_dp[dp, :8, :] = vec_x[0, :8, :] + vec_x[1, :8, :]
    vec_dp[dp, 8:, :] = bias_sum[mine] + vec_x[1, 8:, :]
    send_vec_dp = [copies.new(vec_dp.at[dp], vec_dp.at[dp], peer) for peer in dp_peers]
    for copy in send_vec_dp:
        copy.start()
    for i in range(own_tiles):
        rows = pl.ds(i * TILE, TILE)
        grad_inputs[rows, :] = back_two.take(i) + grad_second[rows, :]
    stores[1].start()
    joint_b.go_third()
    joint_a.go_along()
    joint_c.go_third()
    reduce_inner.go_fourth()
    reduce_outer.done()
    stores[4].start()

    for copy in send_vec_dp:
        copy.wait_recv()
    total = vec_dp[0]
    for index in range(1, dp_size):
        total = total + vec_dp[index]
    vec_z[row] = total
    send_vec_z = [copies.new(vec_z.at[row], vec_z.at[row], peer) for peer in z_peers]
    for copy in send_vec_z:
        copy.start()
    joint_b.go_along()
    joint_c.go_along()
    joint_a.go_fourth()
    reduce_inner.done()
    stores[3].start()
    joint_b.go_fourth()
    joint_c.go_fourth()
    joint_a.done()
    joint_b.done()
    for copy in send_vec_z:
        copy.wait_recv()
    total = vec_z[0]
    for index in range(1, row_size):
        total = total + vec_z[index]
    out_shared[...] = total[:8]
    out_bias[...] = total[8:]
    joint_c.done()
    stores[2].start()
    for store in stores:
        store.wait()
    copies.finish()
    assert len(copies.made) == send_sem.shape[0]


def unpack_kernel(
    layer_in,
    inputs_in,
    joint_in,
    inner_in,
    outer_in,
    shared_in,
    bias_in,
    layer_out,
    inputs_out,
    query_out,
    key_out,
    value_out,
    output_out,
    inner_out,
    outer_out,
    query_bias_out,
    value_bias_out,
    *vectors_out,
):
    piece, width = query_out.shape[1], joint_in.shape[1]
    layer_out[...] = layer_in[...]
    inputs_out[...] = inputs_in[...]
    inner_out[...] = inner_in[...].astype(F32)
    outer_out[...] = outer_in[...].astype(F32)
    joint = joint_in[...].astype(F32)


    def of_kind(rows, which):
        starts = range(piece + which * HEAD_DIM, rows.shape[1], 3 * HEAD_DIM)
        return jnp.concatenate([rows[:, at : at + HEAD_DIM] for at in starts], axis=1)

    output_out[...] = joint[:, :piece]
    for which, out in enumerate((query_out, key_out, value_out)):
        out[...] = of_kind(joint, which)

    @pl.when(pl.program_id(0) == 0)
    def _():
        bias = bias_in[0:1, :]
        query_bias_out[...] = of_kind(bias, 0).reshape(piece)
        value_bias_out[...] = of_kind(bias, 2).reshape(piece)
        for index in range(6):
            vectors_out[index][...] = shared_in[index : index + 1, :].reshape(width)
        vectors_out[6][...] = bias_in[1:2, :].reshape(width)


def shards(
    mesh_shape,
    hidden,
    segments,
    query_weight,
    key_weight,
    value_weight,
    query_bias,
    value_bias,
    output_weight,
    output_bias,
    first_gain,
    first_shift,
    inner_weight,
    inner_bias,
    outer_weight,
    outer_bias,
    second_gain,
    second_shift,
    upstream,
):
    dp_size, row_size, col_size = mesh_shape
    tokens, width = hidden.shape
    length = segments.shape[1]
    block, piece = query_weight.shape
    hidden_units = inner_weight.shape[1]
    heads = piece // HEAD_DIM
    assert col_size == 4 and length == 2 * tokens and 4 * piece == width == hidden_units
    copies_of_gather = 3 * (4 * row_size - 4) - 1
    copies_of_sums = 2 * row_size + row_size // 2 + row_size - 1 + dp_size - 1
    copies_of_vectors = 2 + dp_size - 1 + row_size - 1
    copy_count = 2 + copies_of_gather + 7 * (tokens // TILE) + 5 * copies_of_sums
    copy_count += copies_of_vectors
    half = block // 2
    vmem = pl.BlockSpec(memory_space=pltpu.VMEM)

    def shape(dims, dtype):
        return jax.ShapeDtypeStruct(dims, dtype)

    per_head = pltpu.VMEM((2 * heads, length, HEAD_DIM), BF16)
    weights = pltpu.VMEM((2, width, width), BF16)
    scratch = [
        pltpu.VMEM((tokens, width), BF16),
        pltpu.VMEM((tokens, width), F32),
        pltpu.VMEM((block, width), BF16),
        pltpu.VMEM((block, width), BF16),
        pltpu.VMEM((block, width), BF16),
        pltpu.SemaphoreType.DMA((5,)),
        pltpu.VMEM((block, width), BF16),
        pltpu.VMEM((length, 128), F32),
        pltpu.VMEM((1, length), F32),
        pltpu.VMEM((8, width), F32),
        weights,
        weights,
        weights,
        pltpu.VMEM((length, width), BF16),
        per_head,
        per_head,
        per_head,
        pltpu.VMEM((length, 128), F32),
        per_head,
        pltpu.VMEM((2, length, piece), BF16),
        pltpu.VMEM((2, 8, width), F32),
        pltpu.VMEM((tokens, width), F32),
        pltpu.VMEM((tokens, 1), F32),
        pltpu.VMEM((width, length), BF16),
        pltpu.VMEM((2, length, width), BF16),
        pltpu.VMEM((2, length, width), BF16),
        pltpu.VMEM((length, width), BF16),
        pltpu.VMEM((length, width), BF16),
        per_head,
        pltpu.VMEM((2, tokens, width), BF16),
        pltpu.VMEM((4, tokens, width), BF16),
        pltpu.VMEM((HEAD_DIM, length), BF16),
        pltpu.VMEM((HEAD_DIM, length), BF16),
        pltpu.VMEM((HEAD_DIM, length), F32),
        pltpu.VMEM((HEAD_DIM, length), F32),
        weights,
        weights,
        weights,
        pltpu.VMEM((3, 3 * width // 2, width), BF16),
        pltpu.VMEM((3, row_size - 1, half, width), BF16),
        pltpu.VMEM((3, half, width), BF16),
        pltpu.VMEM((3, dp_size, half, width), BF16),
        pltpu.VMEM((8, width), F32),
        pltpu.VMEM((2, 8, width), F32),
        pltpu.VMEM((8, width), F32),
        pltpu.VMEM((2, 16, width), F32),
        pltpu.VMEM((dp_size, 16, width), F32),
        pltpu.VMEM((row_size, 16, width), F32),
        pltpu.SemaphoreType.DMA((copy_count,)),
        pltpu.SemaphoreType.DMA((copy_count,)),
    ]
    results = pl.pallas_call(
        functools.partial(layer_kernel, (dp_size, row_size)),
        out_shape=[
            shape((tokens, width), BF16),
            shape((tokens, width), F32),
            shape((block, width), BF16),
            shape((block, width), BF16),
            shape((block, width), BF16),
            shape((8, width), F32),
            shape((8, width), F32),
        ],
        in_specs=[vmem] * 18,
        out_specs=[pl.BlockSpec(memory_space=pl.ANY)] * 5 + [vmem] * 2,
        scratch_shapes=scratch,
        compiler_params=pltpu.CompilerParams(
            collective_id=0, has_side_effects=True, vmem_limit_bytes=67043328
        ),
        name="layer",
    )(
        output_weight,
        query_weight,
        key_weight,
        value_weight,
        inner_weight,
        outer_weight,
        hidden,
        upstream,
        segments,
        query_bias,
        value_bias,
        inner_bias,
        output_bias,
        first_gain,
        first_shift,
        outer_bias,
        second_gain,
        second_shift,
    )
    steps = 2

    def part(rows, columns):
        return pl.BlockSpec((rows // steps, columns), lambda i: (i, 0))

    def all_of(rows, columns):
        return pl.BlockSpec((rows, columns), lambda i: (0, 0))

    big = [part(tokens, width)] * 2
    small = [part(block, piece)] * 4
    square = [part(block, width)] * 2
    outs = pl.pallas_call(
        unpack_kernel,
        grid=(steps,),
        out_shape=[shape((tokens, width), BF16), shape((tokens, width), F32)]
        + [shape((block, piece), F32)] * 4
        + [shape((block, width), F32)] * 2
        + [shape((piece,), F32)] * 2
        + [shape((width,), F32)] * 7,
        in_specs=big + [part(block, width)] + square + [all_of(8, width)] * 2,
        out_specs=big + small + square + [pl.BlockSpec((piece,), lambda i: (0,))] * 2
        + [pl.BlockSpec((width,), lambda i: (0,))] * 7,
        name="unpack",
    )(*results)
    layer_out, grad_inputs, grad_query, grad_key, grad_value, grad_output = outs[:6]
    grad_inner, grad_outer = outs[6:8]
    vectors = outs[8:]
    return (
        layer_out,
        grad_inputs,
        grad_query,
        grad_key,
        grad_value,
        vectors[0],
        vectors[1],
        grad_output,
        vectors[2],
        vectors[3],
        vectors[4],
        grad_inner,
        vectors[8],
        grad_outer,
        vectors[5],
        vectors[6],
        vectors[7],
    )


def solution(mesh):
    tokens_spec = P(("dp", "row", "col"), None)
    weight_spec = P("row", "col")
    in_specs = (
        tokens_spec,
        P(("dp", "row"), None),
        weight_spec,
        weight_spec,
        weight_spec,
        P("col"),
        P("col"),
        weight_spec,
        P(),
        P(),
        P(),
        weight_spec,
        P("col"),
        weight_spec,
        P(),
        P(),
        P(),
        tokens_spec,
    )
    out_specs = (
        tokens_spec,
        tokens_spec,
        weight_spec,
        weight_spec,
        weight_spec,
        P("col"),
        P("col"),
        weight_spec,
        P(),
        P(),
        P(),
        weight_spec,
        P("col"),
        weight_spec,
        P(),
        P(),
        P(),
    )
    mesh_shape = (mesh.shape["dp"], mesh.shape["row"], mesh.shape["col"])
    return jax.shard_map(
        functools.partial(shards, mesh_shape),
        mesh=mesh,
        in_specs=in_specs,
        out_specs=out_specs,
        check_vma=False,
    )
```
